128 devices in a mesh: up: 16 (over y_lo, x, core), dn: 8 (over y_hi, z).
Axes of the slice: x: 4, y: 4 (y_hi: 2, y_lo: 2; y = y_hi * 2 + y_lo), z: 4, core: 2. Of those that a mesh axis runs over, the one named last changes fastest.
Arguments:
- start_vector: bfloat16 [13312, 13312], P('up', 'dn'), may hold values from -6 to 6
- hop_tiles: bfloat16 [104, 5, 128, 128], replicated, may hold values from -0.5 to 0.5
- tile_columns: int32 [104, 5], replicated, may hold values from 0 to 103, as said below
- tile_signs: int32 [104, 5], replicated, may hold values from 0 to 1
- occupation: int32 [16, 13312], replicated, may hold values from 0 to 1, as said below
Outputs:
- next_vector: bfloat16 [13312, 13312], P('up', 'dn')
- alphas: float32 [2], replicated
- betas: float32 [2], replicated
The draws below stay inside these ranges and needn't reach their ends.
Inputs may be any that keep to these rules, and one draw needn't show every extreme that they name: Each row of tile_columns names 5 different tile columns. Every column of occupation holds exactly 8 ones.
All inputs are finite; a program needn't handle non-finite values.
Results may differ from the reference program's by a relative error of at most 0.0065.
Values may be sent and summed in bfloat16 or wider, within the bound.
No kernel may reach another device: no remote copies, remote signals or barrier semaphores. Data moves between devices by JAX's collectives and lax.ppermute only.
A program may use at most 192 MiB of HBM per device.

```python
import jax
import jax.numpy as jnp
from jax import lax

DETS = 13312
SITES = 16
TILE = 128
TILE_K = 5
STEPS = 2
TILES = 104


def draw_tile_columns(key, part):
    scores = jax.random.randint(key, (TILES, TILES), 0, 1 << 20) * TILES + jnp.arange(TILES, dtype=jnp.int32)[None, :]
    order = jnp.argsort(scores, axis=1)
    return order[:, :TILE_K].astype(jnp.int32)


def draw_occupation(key, part):
    scores = jax.random.randint(key, (DETS, SITES), 0, 1 << 20) * SITES + jnp.arange(SITES, dtype=jnp.int32)[None, :]
    ranks = jnp.argsort(jnp.argsort(scores, axis=1), axis=1)
    filled = (ranks < SITES // 2).astype(jnp.int32)
    return filled.T


def with_ends(drawn, key, smallest, high):
    dims = drawn.shape
    index_at = [jax.random.randint(jax.random.fold_in(key, axis), (), 0, dims[axis]) for axis in range(len(dims))]
    drawn = drawn.at[tuple(index_at)].set(smallest)
    longest = dims.index(max(dims))
    index_at[longest] = (index_at[longest] + 1) % dims[longest]
    return drawn.at[tuple(index_at)].set(high)


def block_scale(key, dims, shards, smallest, high):
    level = 1.0
    for dim, blocks in shards:
        draws = jax.random.uniform(jax.random.fold_in(jax.random.fold_in(key, 6), dim), (blocks,), jnp.float32, smallest / len(shards), high / len(shards))
        level = level * jnp.repeat(jnp.exp(draws), dims[dim] // blocks).reshape((-1,) + (1,) * (len(dims) - 1 - dim))
    return level


def bell_draw(rng, shape, spread, most, pieces=(), held_as=jnp.bfloat16):
    loudness = block_scale(rng, shape, pieces, -0.22, 0.18) if pieces else 1.0
    entries = jax.random.normal(rng, shape, jnp.float32) * spread * loudness
    return jnp.minimum(jnp.maximum(entries, -most), most).astype(held_as)


def setup_inputs(seed: int = 0) -> dict:
    seeds = jax.random.split(jax.random.key(seed), 6)
    start_vector = bell_draw(seeds[0], (DETS, DETS), 1.0, 6.0, ((0, 16), (1, 8)))
    hop_tiles = bell_draw(seeds[1], (TILES, TILE_K, TILE, TILE), TILE ** -0.5, 0.5)
    tile_columns = draw_tile_columns(jax.random.fold_in(seeds[5], 71), 0)
    tile_signs = with_ends(jax.random.randint(seeds[3], (TILES, TILE_K), 0, 2), jax.random.fold_in(seeds[3], 1), 0, 1).astype(jnp.int32)
    occupation = draw_occupation(jax.random.fold_in(seeds[5], 71), 0)
    return {"start_vector": start_vector, "hop_tiles": hop_tiles, "tile_columns": tile_columns, "tile_signs": tile_signs, "occupation": occupation}


coupling = 4.0

def hop_last(matrix, signed_wide, tile_columns):

    def one_block(part):
        cube = part.reshape(part.shape[0], TILES, TILE)
        picked = cube[:, tile_columns].astype(jnp.float32)
        result = jnp.einsum('ikab,mikb->mia', signed_wide, picked, precision=lax.Precision.HIGHEST)
        return result.reshape(part.shape)
    blocks = matrix.reshape(-1, 512, matrix.shape[1])
    return lax.map(one_block, blocks).reshape(matrix.shape)

def reference(start_vector, hop_tiles, tile_columns, tile_signs, occupation):
    signed = hop_tiles * (1 - 2 * tile_signs).astype(jnp.bfloat16)[:, :, None, None]
    signed_wide = signed.astype(jnp.float32)
    occupied = occupation.astype(jnp.bfloat16)
    diagonal = coupling * jnp.dot(occupied.T, occupied, preferred_element_type=jnp.float32)
    vector = start_vector.astype(jnp.float32)
    total = jnp.sum(vector * vector)
    vector = vector / jnp.maximum(jnp.sqrt(total), 1.0)
    previous = jnp.zeros_like(vector)
    beta_value = jnp.float32(0.0)
    alpha_list = []
    beta_list = []
    for iteration in range(STEPS):
        rounded = vector.astype(jnp.bfloat16)
        hopped_up = hop_last(rounded.T, signed_wide, tile_columns).T.astype(jnp.bfloat16)
        hopped_down = hop_last(rounded, signed_wide, tile_columns).astype(jnp.bfloat16)
        work = hopped_up.astype(jnp.float32) + hopped_down.astype(jnp.float32) + diagonal * vector - beta_value * previous
        intersect = jnp.sum(work * vector)
        work = work - intersect * vector
        residual = jnp.sum(work * work)
        beta_value = jnp.sqrt(jnp.maximum(residual, 1.0))
        previous = vector
        vector = work / beta_value
        alpha_list.append(intersect)
        beta_list.append(beta_value)
    return (vector.astype(jnp.bfloat16), jnp.stack(alpha_list), jnp.stack(beta_list))
```

```python
import jax
import jax.numpy as jnp
from jax import lax
from jax.experimental import pallas as pl
from jax.experimental.pallas import tpu as pltpu
from jax.sharding import Mesh
from jax.sharding import PartitionSpec as P

UP = ("up_0", "up_1", "up_2")
DN = ("dn_0", "dn_1")
ALL = UP + DN
coupling = 4.0

f32 = jnp.float32
bf16 = jnp.bfloat16

T = 128
NT = 104
KT = 5
G = 13
STEPS = NT // G
W = 104
NU = 16
ND = 8
VMEM = 58 * 1024 * 1024


def params():
    return pltpu.CompilerParams(dimension_semantics=("arbitrary",), vmem_limit_bytes=VMEM)


def whole(shape):
    zeros = (0,) * len(shape)
    return pl.BlockSpec(shape, lambda i, *_: zeros, pipeline_mode=pl.Buffered(1))


def tile_spec():
    return pl.BlockSpec((G, KT, T, T), lambda i, *_: (i, 0, 0, 0))


def lane_of(shape):
    return lax.broadcasted_iota(jnp.int32, shape, len(shape) - 1)


def pieces_of(x):
    hi = x.astype(bf16).astype(f32)
    mid = (x - hi).astype(bf16).astype(f32)
    return hi, mid, x - hi - mid


def total_of(x):
    return jnp.sum(jnp.sum(x, axis=0, keepdims=True), axis=1, keepdims=True)


def fold8(x):
    return jnp.sum(x.reshape(x.shape[0] // 8, 8, x.shape[1]), axis=0)


def hop_nat(i, g, idx_ref, tiles_ref, xs):
    row = i * G + g
    left = jnp.concatenate([tiles_ref[g, k] for k in range(KT)], axis=1)
    right = jnp.concatenate([xs[idx_ref[row * KT + k]] for k in range(KT)], axis=0)
    return jnp.dot(left, right, preferred_element_type=f32)


def hop_turned(i, g, idx_ref, tiles_ref, xs):
    row = i * G + g
    right = jnp.concatenate([tiles_ref[g, k] for k in range(KT)], axis=1)
    left = jnp.concatenate([xs[idx_ref[row * KT + k]] for k in range(KT)], axis=1)
    return lax.dot_general(left, right, (((1,), (1,)), ((), ())), preferred_element_type=f32)


def first_up_kernel(idx_ref, a_ref, tiles_ref, occ_rows_ref, occ_cols_ref, p_ref, sums_ref, xs, acc):
    i = pl.program_id(0)

    @pl.when(i == 0)
    def _():
        acc[...] = jnp.zeros_like(acc)

        def put(j, c):
            x = a_ref[j]
            xs[j] = x
            xs[NT + j] = -x
            return c

        lax.fori_loop(0, NT, put, 0)

    for g in range(G):
        row = i * G + g
        p = hop_nat(i, g, idx_ref, tiles_ref, xs).astype(bf16)
        p_ref[row] = p
        a = xs[row].astype(f32)
        diag = coupling * jnp.dot(occ_rows_ref[pl.ds(row * T, T), :], occ_cols_ref[...], preferred_element_type=f32)
        acc[0] += fold8((p.astype(f32) + diag * a) * a)
        acc[1] += fold8(a * a)

    @pl.when(i == STEPS - 1)
    def _():
        energy = total_of(acc[0])
        norm = total_of(acc[1])
        center = (energy / jnp.maximum(norm, 1e-30)).astype(bf16)
        sub = lax.broadcasted_iota(jnp.int32, (8, T), 0)
        sums_ref[...] = jnp.where(sub == 0, energy, jnp.where(sub == 1, norm, center.astype(f32)))
        fill = jnp.broadcast_to(center, (T, T))
        pad = lane_of((T, T)) >= W

        def put(j, c):
            p_ref[j] = jnp.where(pad, fill, p_ref[j])
            return c

        lax.fori_loop(0, NT, put, 0)


def second_up_kernel(idx_ref, a_ref, p_in_ref, tiles_ref, occ_rows_ref, occ_cols_ref, sums_ref, dots_ref, q_ref, xs, extra):
    i = pl.program_id(0)

    @pl.when(i == 0)
    def _():
        energy = sums_ref[0:1, :] + dots_ref[0:1, :]
        norm = sums_ref[1:2, :]
        lane = lane_of((1, T))
        row = jnp.zeros((1, T), f32)
        for k, piece in enumerate(pieces_of(energy) + pieces_of(norm)):
            row = jnp.where(lane == W + k, piece, row)
        extra[...] = jnp.broadcast_to(row, extra.shape)
        center = sums_ref[2:3, :]

        def put(j, c):
            a = a_ref[j].astype(f32)
            diag = coupling * jnp.dot(occ_rows_ref[pl.ds(pl.multiple_of(j * T, T), T), :], occ_cols_ref[...], preferred_element_type=f32)
            x = jnp.where(lane < W, p_in_ref[j].astype(f32) + (diag - center) * a, 0.0).astype(bf16)
            xs[j] = x
            xs[NT + j] = -x
            return c

        lax.fori_loop(0, NT, put, 0)

    pad = lane_of((T, T)) >= W
    for g in range(G):
        q = hop_nat(i, g, idx_ref, tiles_ref, xs)
        q_ref[g] = jnp.where(pad, extra[0:1, :], q).astype(bf16)


def first_down_kernel(idx_ref, a_ref, tiles_ref, r_ref, dots_ref, xs, acc):
    i = pl.program_id(0)

    @pl.when(i == 0)
    def _():
        acc[...] = jnp.zeros_like(acc)

        def put(d, c):
            for o in range(G):
                x = a_ref[d, :, o * T : (o + 1) * T]
                xs[d * G + o] = x
                xs[NT + d * G + o] = -x
            return c

        lax.fori_loop(0, ND, put, 0)

    for g in range(G):
        r = hop_turned(i, g, idx_ref, tiles_ref, xs).astype(bf16)
        r_ref[0, :, g * T : (g + 1) * T] = r
        acc[...] += fold8(r.astype(f32) * xs[i * G + g].astype(f32))

    @pl.when(i == STEPS - 1)
    def _():
        dots_ref[...] = jnp.broadcast_to(total_of(acc[...]), dots_ref.shape)


def pieces_in(o):
    found = []
    for u in range(NU):
        lo, hi = max(u * W, o * T), min((u + 1) * W, (o + 1) * T)
        if lo < hi:
            found.append((u, hi - o * T))
    return found


def assembled(rolled, o, lane):
    found = pieces_in(o)
    value = rolled[found[-1][0]]
    for u, end in reversed(found[:-1]):
        value = jnp.where(lane < end, rolled[u], value)
    return value


def second_down_kernel(idx_ref, a_ref, r_ref, p_ref, tiles_ref, occ_rows_ref, occ_cols_ref, w_ref, t_ref, xs, acc):
    i = pl.program_id(0)

    @pl.when(i == 0)
    def _():
        acc[...] = jnp.zeros_like(acc)
        lane = lane_of((1, T))

        def first(d, c):
            rolled, centers = {}, {}
            done = 0
            for o in range(G):
                for u, _end in pieces_in(o):
                    if u in rolled:
                        continue
                    x = p_ref[u * ND + d].astype(f32)
                    centers[u] = jnp.sum(jnp.where(lane == W, x[0:1, :], 0.0), axis=1, keepdims=True)
                    shift = (u * W) % T
                    rolled[u] = pltpu.roll(x, shift, 1) if shift else x
                p = assembled(rolled, o, lane)
                center = assembled(centers, o, lane)
                lanes = slice(o * T, (o + 1) * T)
                a = a_ref[d, :, lanes].astype(f32)
                r = r_ref[d, :, lanes].astype(f32)
                diag = coupling * jnp.dot(occ_rows_ref[...], occ_cols_ref[d, :, lanes], preferred_element_type=f32)
                w = p + r + diag * a
                w_ref[d, :, lanes] = w
                t_ref[d, :, lanes] = center * p + diag * w
                xs[d * G + o] = p.astype(bf16)
                acc[0] += fold8(w * a)
                acc[1] += fold8(a * a)
            return c

        lax.fori_loop(0, ND, first, 0)
        center = total_of(acc[0]) / jnp.maximum(total_of(acc[1]), 1e-30)

        def second(d, c):
            for o in range(G):
                lanes = slice(o * T, (o + 1) * T)
                a = a_ref[d, :, lanes].astype(f32)
                r = r_ref[d, :, lanes].astype(f32)
                x = (w_ref[d, :, lanes] + xs[d * G + o].astype(f32) - center * a).astype(bf16)
                xs[d * G + o] = x
                xs[NT + d * G + o] = -x
                t_ref[d, :, lanes] += center * r
            return c

        lax.fori_loop(0, ND, second, 0)

    for g in range(G):
        t_ref[i, :, g * T : (g + 1) * T] += hop_turned(i, g, idx_ref, tiles_ref, xs)


def joined_kernel(a_ref, w_ref, t_ref, q_ref, g_ref, sums_ref, acc, scal):
    i = pl.program_id(0)
    lane = lane_of((1, T))

    @pl.when(i == 0)
    def _():
        acc[...] = jnp.zeros_like(acc)

        def add(s, c):
            return c + q_ref[s, 0:8, :].astype(f32)

        row = lax.fori_loop(0, NU * ND, add, jnp.zeros((8, T), f32))[0:1, :]
        energy = jnp.sum(jnp.where((lane >= W) & (lane < W + 3), row, 0.0), axis=1, keepdims=True)
        norm = jnp.sum(jnp.where((lane >= W + 3) & (lane < W + 6), row, 0.0), axis=1, keepdims=True)
        alpha = energy / jnp.maximum(norm, 1.0)
        scal[...] = jnp.where(lane_of(scal.shape) == 0, alpha, norm)

    alpha = scal[0:1, 0:1]
    rolled = {}
    for o in range(G):
        for u, _end in pieces_in(o):
            if u in rolled:
                continue
            x = q_ref[u * ND + i].astype(f32)
            shift = (u * W) % T
            rolled[u] = pltpu.roll(x, shift, 1) if shift else x
        lanes = slice(o * T, (o + 1) * T)
        q = assembled(rolled, o, lane)
        a = a_ref[0, :, lanes].astype(f32)
        w = w_ref[0, :, lanes]
        g = q + t_ref[0, :, lanes]
        g_ref[0, :, lanes] = g
        u = w - alpha * a
        h = g - alpha * (w + u)
        acc[0] += fold8(u * u)
        acc[1] += fold8(u * a)
        acc[2] += fold8(h * h)
        acc[3] += fold8(h * u)
        acc[4] += fold8(h * a)

    @pl.when(i == ND - 1)
    def _():
        row = jnp.where(lane == 5, scal[0:1, 0:1], jnp.where(lane == 6, scal[0:1, 1:2], 0.0))
        for k in range(5):
            row = jnp.where(lane == k, total_of(acc[k]), row)
        sums_ref[...] = jnp.broadcast_to(row, sums_ref.shape)


def final_kernel(coef_ref, a_ref, w_ref, g_ref, v_ref):
    ca, cw, cg = coef_ref[0], coef_ref[1], coef_ref[2]
    v_ref[...] = (cg * g_ref[...] + cw * w_ref[...] + ca * a_ref[...].astype(f32)).astype(bf16)


def body(start_vector, hop_tiles, tile_columns, tile_signs, occupation):
    rows, cols = start_vector.shape
    index = (tile_columns + NT * tile_signs).astype(jnp.int32).reshape(-1)
    up = lax.axis_index(UP)
    down = lax.axis_index(DN)
    occ = occupation.astype(bf16)
    occ_rows = occ.T
    a_cols = lax.dynamic_slice_in_dim(occ, down * cols + up * W, W, 1)
    a_cols = jnp.pad(a_cols, ((0, 0), (0, T - W)))
    b_rows = lax.dynamic_slice_in_dim(occ_rows, up * rows + down * W, W, 0)
    b_cols = jnp.moveaxis(occ.reshape(occ.shape[0], ND, cols), 1, 0)

    parts = [jnp.pad(start_vector[:, k * W : (k + 1) * W], ((0, 0), (0, T - W))) for k in range(NU)]
    a_up = lax.all_to_all(jnp.stack(parts), UP, 0, 0, tiled=True).reshape(NT, T, T)
    a_up, start_later = lax.optimization_barrier((a_up, start_vector))
    a_dn = lax.all_to_all(start_later.reshape(ND, W, cols), DN, 0, 0, tiled=True)

    hop_flops = 2 * NT * KT * T * T * T
    tile_bytes = NT * KT * T * T * 2
    cost = pl.CostEstimate(flops=hop_flops, bytes_accessed=tile_bytes + 8 * 2**20, transcendentals=0)
    nat = (NT, T, T)
    wide = (ND, W, cols)
    xs_nat = pltpu.VMEM((2 * NT, T, T), bf16)
    xs_turned = pltpu.VMEM((2 * NT, W, T), bf16)

    p, sums = pl.pallas_call(
        first_up_kernel,
        grid_spec=pltpu.PrefetchScalarGridSpec(
            num_scalar_prefetch=1,
            grid=(STEPS,),
            in_specs=[whole(nat), tile_spec(), whole(occ_rows.shape), whole(a_cols.shape)],
            out_specs=[whole(nat), whole((8, T))],
            scratch_shapes=[xs_nat, pltpu.VMEM((2, 8, T), f32)],
        ),
        out_shape=[jax.ShapeDtypeStruct(nat, bf16), jax.ShapeDtypeStruct((8, T), f32)],
        compiler_params=params(),
        cost_estimate=cost,
        name="first_up",
    )(index, a_up, hop_tiles, occ_rows, a_cols)

    p_dn = lax.all_to_all(p.reshape(NU * ND, W, T), ALL, 0, 0, tiled=True)

    r, dots = pl.pallas_call(
        first_down_kernel,
        grid_spec=pltpu.PrefetchScalarGridSpec(
            num_scalar_prefetch=1,
            grid=(STEPS,),
            in_specs=[whole(wide), tile_spec()],
            out_specs=[pl.BlockSpec((1, W, cols), lambda i, *_: (i, 0, 0)), whole((8, T))],
            scratch_shapes=[xs_turned, pltpu.VMEM((8, T), f32)],
        ),
        out_shape=[jax.ShapeDtypeStruct(wide, bf16), jax.ShapeDtypeStruct((8, T), f32)],
        compiler_params=params(),
        cost_estimate=cost,
        name="first_down",
    )(index, a_dn, hop_tiles)

    q = pl.pallas_call(
        second_up_kernel,
        grid_spec=pltpu.PrefetchScalarGridSpec(
            num_scalar_prefetch=1,
            grid=(STEPS,),
            in_specs=[
                whole(nat),
                whole(nat),
                tile_spec(),
                whole(occ_rows.shape),
                whole(a_cols.shape),
                whole((8, T)),
                whole((8, T)),
            ],
            out_specs=pl.BlockSpec((G, T, T), lambda i, *_: (i, 0, 0)),
            scratch_shapes=[xs_nat, pltpu.VMEM((8, T), f32)],
        ),
        out_shape=jax.ShapeDtypeStruct(nat, bf16),
        compiler_params=params(),
        cost_estimate=cost,
        name="second_up",
    )(index, a_up, p, hop_tiles, occ_rows, a_cols, sums, dots)

    p_dn, q = lax.optimization_barrier((p_dn, q))
    q_dn = lax.all_to_all(q.reshape(NU * ND, W, T), ALL, 0, 0, tiled=True)

    w, t = pl.pallas_call(
        second_down_kernel,
        grid_spec=pltpu.PrefetchScalarGridSpec(
            num_scalar_prefetch=1,
            grid=(STEPS,),
            in_specs=[
                whole(wide),
                whole(wide),
                whole((NU * ND, W, T)),
                tile_spec(),
                whole(b_rows.shape),
                whole(b_cols.shape),
            ],
            out_specs=[whole(wide), whole(wide)],
            scratch_shapes=[xs_turned, pltpu.VMEM((2, 8, T), f32)],
        ),
        out_shape=[jax.ShapeDtypeStruct(wide, f32), jax.ShapeDtypeStruct(wide, f32)],
        compiler_params=params(),
        cost_estimate=cost,
        name="second_down",
    )(index, a_dn, r, p_dn, hop_tiles, b_rows, b_cols)

    block = pl.BlockSpec((1, W, cols), lambda i, *_: (i, 0, 0))
    g, partial = pl.pallas_call(
        joined_kernel,
        grid=(ND,),
        in_specs=[block, block, block, whole((NU * ND, W, T))],
        out_specs=[block, whole((NU * ND, T))],
        out_shape=[jax.ShapeDtypeStruct(wide, f32), jax.ShapeDtypeStruct((NU * ND, T), f32)],
        scratch_shapes=[pltpu.VMEM((5, 8, T), f32), pltpu.VMEM((8, T), f32)],
        compiler_params=params(),
        name="joined",
    )(a_dn, w, t, q_dn)

    shared = lax.all_to_all(partial, ALL, 0, 0, tiled=True)
    uu, ua, hh, hu, ha, _alpha, _norm = [jnp.sum(shared[:, k]) for k in range(7)]
    alpha1 = partial[0, 5]
    norm = partial[0, 6]
    scale2 = 1.0 / jnp.maximum(norm, 1.0)
    square1 = jnp.maximum(scale2 * uu, 1.0)
    beta1 = jnp.sqrt(square1)
    ratio2 = scale2 / square1
    alpha2 = ratio2 * (hu + alpha1 * uu - square1 * ua)
    shift = alpha2 - alpha1
    nn = hh + square1 * square1 * norm + shift * shift * uu - 2.0 * square1 * ha - 2.0 * shift * hu + 2.0 * square1 * shift * ua
    square2 = jnp.maximum(ratio2 * nn, 1.0)
    beta2 = jnp.sqrt(square2)
    cg = jnp.sqrt(ratio2) / beta2
    cw = -cg * (alpha1 + alpha2)
    ca = cg * (alpha1 * alpha2 - square1)
    coef = jnp.stack([ca, cw, cg])

    v = pl.pallas_call(
        final_kernel,
        grid_spec=pltpu.PrefetchScalarGridSpec(
            num_scalar_prefetch=1,
            grid=(ND,),
            in_specs=[block, block, block],
            out_specs=block,
        ),
        out_shape=jax.ShapeDtypeStruct(wide, bf16),
        compiler_params=params(),
        name="final",
    )(coef, a_dn, w, g)
    final = lax.all_to_all(v, DN, 0, 0, tiled=True).reshape(rows, cols)
    return final, jnp.stack([alpha1, alpha2]), jnp.stack([beta1, beta2])


def solution(mesh):
    torus = Mesh(mesh.devices.reshape(2, 4, 2, 2, 4), ALL)
    return jax.shard_map(
        body,
        mesh=torus,
        in_specs=(P(UP, DN), P(), P(), P(), P()),
        out_specs=(P(UP, DN), P(), P()),
        check_vma=False,
    )
```

```python
import jax
import jax.numpy as jnp
from jax import lax
from jax.experimental import pallas as pl
from jax.experimental.pallas import tpu as pltpu
from jax.sharding import Mesh
from jax.sharding import PartitionSpec as P


UP = ("up_0", "up_1", "up_2")
DN = ("dn_0", "dn_1")
ALL = UP + DN
coupling = 4.0

f32 = jnp.float32
bf16 = jnp.bfloat16

T = 128
NT = 104
KT = 5
G = 13
STEPS = NT // G
W = 104
NU = 16
ND = 8
MIB = 1024 * 1024


def params(mib):
    return pltpu.CompilerParams(dimension_semantics=("arbitrary",), vmem_limit_bytes=mib * MIB)


def whole(shape):
    zeros = (0,) * len(shape)
    return pl.BlockSpec(shape, lambda i, *_: zeros, pipeline_mode=pl.Buffered(1))


def tile_spec():
    return pl.BlockSpec((G, KT, T, T), lambda i, *_: (i, 0, 0, 0))


def lane_of(shape):
    return lax.broadcasted_iota(jnp.int32, shape, len(shape) - 1)


def pieces_of(x):
    hi = x.astype(bf16).astype(f32)
    mid = (x - hi).astype(bf16).astype(f32)
    return hi, mid, x - hi - mid


def total_of(x):
    return jnp.sum(jnp.sum(x, axis=0, keepdims=True), axis=1, keepdims=True)


def fold8(x):
    return jnp.sum(x.reshape(x.shape[0] // 8, 8, x.shape[1]), axis=0)


def hop_nat(i, g, idx_ref, tiles_ref, xs):
    row = i * G + g
    left = jnp.concatenate([tiles_ref[g, k] for k in range(KT)], axis=1)
    right = [xs[pl.ds(pl.multiple_of(idx_ref[row * KT + k] * T, T), T), :] for k in range(KT)]
    return jnp.dot(left, jnp.concatenate(right, axis=0), preferred_element_type=f32)


def hop_turned(i, g, idx_ref, tiles_ref, xs):
    row = i * G + g
    right = jnp.concatenate([tiles_ref[g, k] for k in range(KT)], axis=1)
    left = jnp.concatenate([xs[idx_ref[row * KT + k]] for k in range(KT)], axis=1)
    return lax.dot_general(left, right, (((1,), (1,)), ((), ())), preferred_element_type=f32)


LOW = T - W
STRIPS = -(-W // LOW)


def turned(x, shift):
    shift %= T
    return pltpu.roll(x, shift, 1) if shift else x


def with_strip(head, tail, k, lane):
    return jnp.where(lane < W, head, turned(tail, W - LOW * k))


def from_strips(strips, lane):
    value = turned(strips[-1], LOW * (STRIPS - 1) - W)
    for k in reversed(range(STRIPS - 1)):
        value = jnp.where(lane < LOW * (k + 1), turned(strips[k], LOW * k - W), value)
    return value


ROWS = 832
HEAD = 704
H = 64
WH = 88
S = W - WH


def pack_kernel(a_ref, out_ref):
    lane = lane_of((1, T))

    def cut(u, block):
        q, o = divmod(u * W, T)
        rows = slice(block * H, (block + 1) * H)
        x = turned(a_ref[rows, q * T : (q + 1) * T].astype(f32), -o)
        if o + W > T:
            y = turned(a_ref[rows, (q + 1) * T : (q + 2) * T].astype(f32), -o)
            x = jnp.where(lane < T - o, x, y)
        return x

    for u in range(NU):
        tails = [cut(u, HEAD // H + h) for h in range(2)]
        for block in range(HEAD // H):
            x = cut(u, block)
            if block < 2 * STRIPS:
                x = with_strip(x, tails[block % 2], block // 2, lane)
            out_ref[u, block * H : (block + 1) * H, :] = x.astype(bf16)


def packed(values, t, lane):
    x = values[pl.ds(pl.multiple_of(t * W, 8), WH), :]
    tail = values[pl.ds(pl.multiple_of(t * W + WH, 8), S), :]
    found = [with_strip(x[S * k : S * (k + 1)], tail, k, lane) for k in range(STRIPS)]
    return jnp.concatenate(found + [x[S * STRIPS :]], axis=0)


def unpacked(x, lane):
    tail = from_strips([x[S * k : S * (k + 1)] for k in range(STRIPS)], lane)
    return jnp.concatenate([x, tail], axis=0)


FREE = S * (STRIPS - 1)
FREE_LANE = W + W - LOW * (STRIPS - 1)


def first_up_kernel(idx_ref, a_ref, tiles_ref, occ_rows_ref, occ_cols_ref, p_ref, x_ref, sums_ref, xs, whole_w, some_p, acc):
    i = pl.program_id(0)
    lane = lane_of((1, T))

    @pl.when(i == 0)
    def _():
        acc[...] = jnp.zeros_like(acc)

        def put(s, c):
            def keep(row, x):
                x = jnp.where(lane < W, x, 0.0).astype(bf16)
                at = pl.multiple_of(s * ROWS + row, H)
                xs[pl.ds(at, H), :] = x
                xs[pl.ds(NT * T + at, H), :] = -x

            for block in range(HEAD // H):
                keep(block * H, a_ref[s, block * H : (block + 1) * H, :].astype(f32))
            for h in range(2):
                strips = [
                    a_ref[s, (2 * k + h) * H : (2 * k + h + 1) * H, :].astype(f32) for k in range(STRIPS)
                ]
                keep(HEAD + h * H, from_strips(strips, lane))
            return c

        lax.fori_loop(0, NU, put, 0)

    for g in range(G):
        rows = pl.ds(pl.multiple_of((i * G + g) * T, T), T)
        p = hop_nat(i, g, idx_ref, tiles_ref, xs).astype(bf16).astype(f32)
        some_p[g * T : (g + 1) * T, :] = p
        a = xs[rows, :].astype(f32)
        diag = coupling * jnp.dot(occ_rows_ref[rows, :], occ_cols_ref[...], preferred_element_type=f32)
        w = p + diag * a
        whole_w[rows, :] = w
        acc[0] += fold8(w * a)
        acc[1] += fold8(a * a)
    for t in range(NU):
        p_ref[i * NU + t] = packed(some_p, t, lane).astype(bf16)

    @pl.when(i == STEPS - 1)
    def _():
        energy = total_of(acc[0])
        norm = total_of(acc[1])
        center = (energy / jnp.maximum(norm, 1e-30)).astype(bf16)
        sub = lax.broadcasted_iota(jnp.int32, (8, T), 0)
        sums_ref[...] = jnp.where(sub == 0, energy, norm)
        fill = jnp.broadcast_to(center, (S, T))
        free = lane_of((S, T)) >= FREE_LANE

        def mark(s, c):
            p_ref[s, FREE : FREE + S, :] = jnp.where(free, fill, p_ref[s, FREE : FREE + S, :])
            return c

        lax.fori_loop(0, NU * ND, mark, 0)
        wide = center.astype(f32)

        def put(j, c):
            rows = pl.ds(pl.multiple_of(j * T, T), T)
            x_ref[rows, :] = (whole_w[rows, :] - wide * xs[rows, :].astype(f32)).astype(bf16)
            return c

        lax.fori_loop(0, NT, put, 0)


def second_up_kernel(idx_ref, x_ref, tiles_ref, sums_ref, dots_ref, q_ref, xs, some_q, extra):
    i = pl.program_id(0)
    lane = lane_of((1, T))

    @pl.when(i == 0)
    def _():
        energy = sums_ref[0:1, :] + dots_ref[0:1, :]
        norm = sums_ref[1:2, :]
        row = jnp.zeros((1, T), f32)
        for k, piece in enumerate(pieces_of(energy) + pieces_of(norm)):
            row = jnp.where(lane == FREE_LANE + k, piece, row)
        extra[...] = jnp.broadcast_to(row, extra.shape)

        def put(j, c):
            at = pl.multiple_of(j * T, T)
            x = x_ref[pl.ds(at, T), :]
            xs[pl.ds(at, T), :] = x
            xs[pl.ds(NT * T + at, T), :] = -x
            return c

        lax.fori_loop(0, NT, put, 0)

    for g in range(G):
        some_q[g * T : (g + 1) * T, :] = hop_nat(i, g, idx_ref, tiles_ref, xs)
    for t in range(NU):
        x = packed(some_q, t, lane)
        marked = jnp.where(lane >= FREE_LANE, extra[0:1, :], x[FREE : FREE + S])
        q_ref[t] = jnp.concatenate([x[:FREE], marked, x[FREE + S :]], axis=0).astype(bf16)


def first_down_kernel(idx_ref, a_ref, tiles_ref, r_ref, dots_ref, xs, acc):
    i = pl.program_id(0)

    @pl.when(i == 0)
    def _():
        acc[...] = jnp.zeros_like(acc)

        def put(d, c):
            for o in range(G):
                x = a_ref[d, :, o * T : (o + 1) * T]
                xs[d * G + o] = x
                xs[NT + d * G + o] = -x
            return c

        lax.fori_loop(0, ND, put, 0)

    for g in range(G):
        r = hop_turned(i, g, idx_ref, tiles_ref, xs).astype(bf16)
        r_ref[0, :, g * T : (g + 1) * T] = r
        acc[...] += fold8(r.astype(f32) * xs[i * G + g].astype(f32))

    @pl.when(i == STEPS - 1)
    def _():
        dots_ref[...] = jnp.broadcast_to(total_of(acc[...]), dots_ref.shape)


def pieces_in(o):
    found = []
    for u in range(NU):
        lo, hi = max(u * W, o * T), min((u + 1) * W, (o + 1) * T)
        if lo < hi:
            found.append((u, hi - o * T))
    return found


def assembled(rolled, o, lane):
    found = pieces_in(o)
    value = rolled[found[-1][0]]
    for u, end in reversed(found[:-1]):
        value = jnp.where(lane < end, rolled[u], value)
    return value


def second_down_kernel(idx_ref, a_ref, r_ref, p_ref, tiles_ref, occ_rows_ref, occ_cols_ref, u_ref, t_ref, center_ref, xs, w_ref, acc):
    i = pl.program_id(0)

    @pl.when(i == 0)
    def _():
        acc[...] = jnp.zeros_like(acc)
        lane = lane_of((1, T))

        def first(d, c):
            rolled, centers = {}, {}
            for o in range(G):
                for u, _end in pieces_in(o):
                    if u in rolled:
                        continue
                    x = p_ref[u * ND + d].astype(f32)
                    centers[u] = jnp.sum(jnp.where(lane == FREE_LANE, x[FREE : FREE + 1, :], 0.0), axis=1, keepdims=True)
                    rolled[u] = turned(unpacked(x, lane), u * W)
                p = assembled(rolled, o, lane)
                center = assembled(centers, o, lane)
                lanes = slice(o * T, (o + 1) * T)
                a = a_ref[d, :, lanes].astype(f32)
                r = r_ref[d, :, lanes].astype(f32)
                diag = coupling * jnp.dot(occ_rows_ref[...], occ_cols_ref[d, :, lanes], preferred_element_type=f32)
                w = p + r + diag * a
                w_ref[d, :, lanes] = w
                t_ref[d, :, lanes] = center * p + diag * w
                xs[d * G + o] = p.astype(bf16)
                acc[0] += fold8(w * a)
                acc[1] += fold8(a * a)
            return c

        lax.fori_loop(0, ND, first, 0)
        center = total_of(acc[0]) / jnp.maximum(total_of(acc[1]), 1e-30)
        center_ref[...] = jnp.broadcast_to(center, center_ref.shape)

        def second(d, c):
            for o in range(G):
                lanes = slice(o * T, (o + 1) * T)
                a = a_ref[d, :, lanes].astype(f32)
                r = r_ref[d, :, lanes].astype(f32)
                w = w_ref[d, :, lanes]
                u = w - center * a
                u_ref[d, :, lanes] = u.astype(bf16)
                x = (u + xs[d * G + o].astype(f32)).astype(bf16)
                xs[d * G + o] = x
                xs[NT + d * G + o] = -x
                t_ref[d, :, lanes] += center * (r - w - u)
            return c

        lax.fori_loop(0, ND, second, 0)

    for g in range(G):
        t_ref[i, :, g * T : (g + 1) * T] += hop_turned(i, g, idx_ref, tiles_ref, xs)


def joined_kernel(a_ref, u_ref, t_ref, q_ref, center_ref, g_ref, sums_ref, acc, scal):
    i = pl.program_id(0)
    lane = lane_of((1, T))

    @pl.when(i == 0)
    def _():
        acc[...] = jnp.zeros_like(acc)

        def add(s, c):
            for k in range(8):
                c = c + q_ref[s * 8 + k, FREE : FREE + S, :].astype(f32)
            return c

        row = lax.fori_loop(0, NU * ND // 8, add, jnp.zeros((S, T), f32))[0:1, :]
        first = (lane >= FREE_LANE) & (lane < FREE_LANE + 3)
        second = (lane >= FREE_LANE + 3) & (lane < FREE_LANE + 6)
        energy = jnp.sum(jnp.where(first, row, 0.0), axis=1, keepdims=True)
        norm = jnp.sum(jnp.where(second, row, 0.0), axis=1, keepdims=True)
        alpha = energy / jnp.maximum(norm, 1.0)
        scal[...] = jnp.where(lane_of(scal.shape) == 0, alpha, norm)

    off = center_ref[0:1, 0:1] - scal[0:1, 0:1]
    rolled = {}
    for o in range(G):
        for u, _end in pieces_in(o):
            if u not in rolled:
                rolled[u] = turned(unpacked(q_ref[u * ND + i].astype(f32), lane), u * W)
        lanes = slice(o * T, (o + 1) * T)
        q = assembled(rolled, o, lane)
        a = a_ref[0, :, lanes].astype(f32)
        near = u_ref[0, :, lanes].astype(f32)
        g = q + t_ref[0, :, lanes]
        g_ref[i, :, lanes] = g
        u = near + off * a
        h = g + off * (near + u)
        acc[0] += fold8(u * u)
        acc[1] += fold8(u * a)
        acc[2] += fold8(h * h)
        acc[3] += fold8(h * u)
        acc[4] += fold8(h * a)

    @pl.when(i == ND - 1)
    def _():
        row = jnp.where(lane == 5, scal[0:1, 0:1], jnp.where(lane == 6, scal[0:1, 1:2], 0.0))
        for k in range(5):
            row = jnp.where(lane == k, total_of(acc[k]), row)
        sums_ref[...] = jnp.broadcast_to(row, sums_ref.shape)


def final_kernel(a_ref, u_ref, g_ref, center_ref, shared_ref, v_ref, out_ref, coef):
    i = pl.program_id(0)
    lane = lane_of((1, T))

    @pl.when(i == 0)
    def _():
        sums = jnp.sum(shared_ref[...], axis=0, keepdims=True)
        own = shared_ref[0:1, :]

        def pick(row, k):
            return jnp.sum(jnp.where(lane == k, row, 0.0), axis=1, keepdims=True)

        uu, ua, hh, hu, ha = [pick(sums, k) for k in range(5)]
        alpha1, norm = pick(own, 5), pick(own, 6)
        scale2 = 1.0 / jnp.maximum(norm, 1.0)
        square1 = jnp.maximum(scale2 * uu, 1.0)
        ratio2 = scale2 / square1
        alpha2 = ratio2 * (hu + alpha1 * uu - square1 * ua)
        move = alpha2 - alpha1
        nn = hh + square1 * square1 * norm + move * move * uu
        nn = nn - 2.0 * square1 * ha - 2.0 * move * hu + 2.0 * square1 * move * ua
        square2 = jnp.maximum(ratio2 * nn, 1.0)
        beta1, beta2 = jnp.sqrt(square1), jnp.sqrt(square2)
        cg = jnp.sqrt(ratio2) / beta2
        row = jnp.zeros((1, T), f32)
        off = center_ref[0:1, 0:1] - alpha1
        for k, value in enumerate(
            [alpha1, alpha2, beta1, beta2, cg * (off * (off - move) - square1), cg * (2.0 * off - move), cg]
        ):
            row = jnp.where(lane == k, value, row)
        coef[...] = jnp.broadcast_to(row, coef.shape)
        out_ref[...] = jnp.broadcast_to(row, out_ref.shape)

    ca, cu, cg = coef[0:1, 4:5], coef[0:1, 5:6], coef[0:1, 6:7]
    v_ref[0] = (cg * g_ref[i] + cu * u_ref[0].astype(f32) + ca * a_ref[0].astype(f32)).astype(bf16)


def swapped_down(start_vector):
    down = lax.axis_index(DN)
    cols = start_vector.shape[1]
    joined = jnp.zeros((ND, W, cols), start_vector.dtype)
    for s in range(ND):
        piece = lax.dynamic_slice_in_dim(start_vector, (down + s) % ND * W, W, 0)
        if s:
            piece = lax.ppermute(piece, DN, [(k, (k + s) % ND) for k in range(ND)])
        joined = lax.dynamic_update_slice(joined, piece[None], ((down - s) % ND, 0, 0))
    return joined


def body(start_vector, hop_tiles, tile_columns, tile_signs, occupation):
    rows, cols = start_vector.shape
    index = (tile_columns + NT * tile_signs).astype(jnp.int32).reshape(-1)
    up = lax.axis_index(UP)
    down = lax.axis_index(DN)
    occ = occupation.astype(bf16)
    occ_rows = occ.T
    a_cols = lax.dynamic_slice_in_dim(occ, down * cols + up * W, W, 1)
    a_cols = jnp.pad(a_cols, ((0, 0), (0, T - W)))
    b_rows = lax.dynamic_slice_in_dim(occ_rows, up * rows + down * W, W, 0)
    b_cols = jnp.moveaxis(occ.reshape(occ.shape[0], ND, cols), 1, 0)

    parts = pl.pallas_call(
        pack_kernel,
        out_shape=pltpu.HBM((NU, HEAD, T), bf16),
        compiler_params=pltpu.CompilerParams(vmem_limit_bytes=24 * MIB),
        name="pack",
    )(pltpu.with_memory_space_constraint(start_vector, pltpu.HBM))
    a_up = lax.all_to_all(parts, UP, 0, 0, tiled=True)
    a_dn = swapped_down(start_vector)

    hop_flops = 2 * NT * KT * T * T * T
    tile_bytes = NT * KT * T * T * 2
    cost = pl.CostEstimate(flops=hop_flops, bytes_accessed=tile_bytes + 8 * 2**20, transcendentals=0)
    tall = (NT * T, T)
    packs = (NU * ND, WH, T)
    wide = (ND, W, cols)
    xs_tall = pltpu.VMEM((2 * NT * T, T), bf16)
    some = pltpu.VMEM((G * T, T), f32)
    xs_turned = pltpu.VMEM((2 * NT, W, T), bf16)

    first_up = pl.pallas_call(
        first_up_kernel,
        grid_spec=pltpu.PrefetchScalarGridSpec(
            num_scalar_prefetch=1,
            grid=(STEPS,),
            in_specs=[whole((NU, HEAD, T)), tile_spec(), whole(occ_rows.shape), whole(a_cols.shape)],
            out_specs=[whole(packs), whole(tall), whole((8, T))],
            scratch_shapes=[xs_tall, pltpu.VMEM(tall, f32), some, pltpu.VMEM((2, 8, T), f32)],
        ),
        out_shape=[
            pltpu.HBM(packs, bf16),
            pltpu.HBM(tall, bf16),
            jax.ShapeDtypeStruct((8, T), f32),
        ],
        compiler_params=params(44),
        cost_estimate=cost,
        name="first_up",
    )
    p, x, sums = first_up(index, a_up, hop_tiles, occ_rows, a_cols)

    p_dn = lax.all_to_all(p, ALL, 0, 0, tiled=True)

    r, dots = pl.pallas_call(
        first_down_kernel,
        grid_spec=pltpu.PrefetchScalarGridSpec(
            num_scalar_prefetch=1,
            grid=(STEPS,),
            in_specs=[whole(wide), tile_spec()],
            out_specs=[pl.BlockSpec((1, W, cols), lambda i, *_: (i, 0, 0)), whole((8, T))],
            scratch_shapes=[xs_turned, pltpu.VMEM((8, T), f32)],
        ),
        out_shape=[pltpu.HBM(wide, bf16), jax.ShapeDtypeStruct((8, T), f32)],
        compiler_params=params(32),
        cost_estimate=cost,
        name="first_down",
    )(index, a_dn, hop_tiles)

    q = pl.pallas_call(
        second_up_kernel,
        grid_spec=pltpu.PrefetchScalarGridSpec(
            num_scalar_prefetch=1,
            grid=(STEPS,),
            in_specs=[whole(tall), tile_spec(), whole((8, T)), whole((8, T))],
            out_specs=pl.BlockSpec((NU, WH, T), lambda i, *_: (i, 0, 0)),
            scratch_shapes=[xs_tall, some, pltpu.VMEM((8, T), f32)],
        ),
        out_shape=pltpu.HBM(packs, bf16),
        compiler_params=params(32),
        cost_estimate=cost,
        name="second_up",
    )(index, x, hop_tiles, sums, dots)

    p_dn, q = lax.optimization_barrier((p_dn, q))
    q_dn = lax.all_to_all(q, ALL, 0, 0, tiled=True)

    near = pl.BlockSpec(memory_space=pltpu.VMEM)
    kept = pltpu.VMEM(wide, f32)
    u, t, center = pl.pallas_call(
        second_down_kernel,
        grid_spec=pltpu.PrefetchScalarGridSpec(
            num_scalar_prefetch=1,
            grid=(STEPS,),
            in_specs=[
                whole(wide),
                whole(wide),
                whole(packs),
                tile_spec(),
                whole(b_rows.shape),
                whole(b_cols.shape),
            ],
            out_specs=[whole(wide), whole(wide), whole((8, T))],
            scratch_shapes=[xs_turned, kept, pltpu.VMEM((2, 8, T), f32)],
        ),
        out_shape=[pltpu.HBM(wide, bf16), pltpu.HBM(wide, f32), jax.ShapeDtypeStruct((8, T), f32)],
        compiler_params=params(48),
        cost_estimate=cost,
        name="second_down",
    )(index, a_dn, r, p_dn, hop_tiles, b_rows, b_cols)

    block = pl.BlockSpec((1, W, cols), lambda i, *_: (i, 0, 0))
    g, partial = pl.pallas_call(
        joined_kernel,
        grid=(ND,),
        in_specs=[block, block, block, whole(packs), whole((8, T))],
        out_specs=[near, whole((NU * ND, T))],
        out_shape=[kept, jax.ShapeDtypeStruct((NU * ND, T), f32)],
        scratch_shapes=[pltpu.VMEM((5, 8, T), f32), pltpu.VMEM((8, T), f32)],
        compiler_params=params(20),
        name="joined",
    )(a_dn, u, t, q_dn, center)

    shared = lax.all_to_all(partial, ALL, 0, 0, tiled=True)
    v, scalars = pl.pallas_call(
        final_kernel,
        grid=(ND,),
        in_specs=[block, block, near, whole((8, T)), whole((NU * ND, T))],
        out_specs=[block, whole((8, T))],
        out_shape=[pltpu.HBM(wide, bf16), jax.ShapeDtypeStruct((8, T), f32)],
        scratch_shapes=[pltpu.VMEM((8, T), f32)],
        compiler_params=params(16),
        name="final",
    )(a_dn, u, g, center, shared)
    final = lax.all_to_all(v, DN, 0, 0, tiled=True).reshape(rows, cols)
    return final, scalars[0, 0:2], scalars[0, 2:4]


def solution(mesh):
    torus = Mesh(mesh.devices.reshape(2, 4, 2, 2, 4), ALL)
    return jax.shard_map(
        body,
        mesh=torus,
        in_specs=(P(UP, DN), P(), P(), P(), P()),
        out_specs=(P(UP, DN), P(), P()),
        check_vma=False,
    )
```

```python
import jax
import jax.numpy as jnp
from jax import lax
from jax.experimental import pallas as pl
from jax.experimental.pallas import tpu as pltpu
from jax.sharding import Mesh
from jax.sharding import PartitionSpec as P


UP = ("up_0", "up_1", "up_2")
DN = ("dn_0", "dn_1")
ALL = UP + DN
coupling = 4.0

f32 = jnp.float32
bf16 = jnp.bfloat16

T = 128
NT = 104
KT = 5
G = 13
STEPS = NT // G
W = 104
NU = 16
ND = 8
MIB = 1024 * 1024


def params(mib):
    return pltpu.CompilerParams(dimension_semantics=("arbitrary",), vmem_limit_bytes=mib * MIB)


def whole(shape):
    zeros = (0,) * len(shape)
    return pl.BlockSpec(shape, lambda i, *_: zeros, pipeline_mode=pl.Buffered(1))


def far(x):
    return pltpu.with_memory_space_constraint(x, pltpu.HBM)


def tile_spec():
    return pl.BlockSpec((G, KT, T, T), lambda i, *_: (i, 0, 0, 0))


def lane_of(shape):
    return lax.broadcasted_iota(jnp.int32, shape, len(shape) - 1)


def total_of(x):
    return jnp.sum(jnp.sum(x, axis=0, keepdims=True), axis=1, keepdims=True)


def fold8(x):
    return jnp.sum(x.reshape(x.shape[0] // 8, 8, x.shape[1]), axis=0)


def hop_nat(i, g, idx_ref, tiles_ref, xs):
    row = i * G + g
    left = jnp.concatenate([tiles_ref[g, k] for k in range(KT)], axis=1)
    right = [xs[pl.ds(pl.multiple_of(idx_ref[row * KT + k] * T, T), T), :] for k in range(KT)]
    return jnp.dot(left, jnp.concatenate(right, axis=0), preferred_element_type=f32)


def hop_turned(row, idx_ref, tiles, xs):
    right = jnp.concatenate([tiles[row, k] for k in range(KT)], axis=1)
    left = jnp.concatenate([xs[idx_ref[row * KT + k]] for k in range(KT)], axis=1)
    return lax.dot_general(left, right, (((1,), (1,)), ((), ())), preferred_element_type=f32)


LOW = T - W
STRIPS = -(-W // LOW)


def turned(x, shift):
    shift %= T
    return pltpu.roll(x, shift, 1) if shift else x


def with_strip(head, tail, k, lane):
    return jnp.where(lane < W, head, turned(tail, W - LOW * k))


def from_strips(strips, lane):
    value = turned(strips[-1], LOW * (STRIPS - 1) - W)
    for k in reversed(range(STRIPS - 1)):
        value = jnp.where(lane < LOW * (k + 1), turned(strips[k], LOW * k - W), value)
    return value


ROWS = 832
HEAD = 704
H = 64
WH = 88
S = W - WH


def pack_kernel(a_ref, out_ref):
    lane = lane_of((1, T))

    def cut(u, block):
        q, o = divmod(u * W, T)
        rows = slice(block * H, (block + 1) * H)
        x = turned(a_ref[rows, q * T : (q + 1) * T].astype(f32), -o)
        if o + W > T:
            y = turned(a_ref[rows, (q + 1) * T : (q + 2) * T].astype(f32), -o)
            x = jnp.where(lane < T - o, x, y)
        return x

    for u in range(NU):
        tails = [cut(u, HEAD // H + h) for h in range(2)]
        for block in range(HEAD // H):
            x = cut(u, block)
            if block < 2 * STRIPS:
                x = with_strip(x, tails[block % 2], block // 2, lane)
            out_ref[u, block * H : (block + 1) * H, :] = x.astype(bf16)


def packed(values, t, lane):
    x = values[pl.ds(pl.multiple_of(t * W, 8), WH), :]
    tail = values[pl.ds(pl.multiple_of(t * W + WH, 8), S), :]
    found = [with_strip(x[S * k : S * (k + 1)], tail, k, lane) for k in range(STRIPS)]
    return jnp.concatenate(found + [x[S * STRIPS :]], axis=0)


def unpacked(x, lane):
    tail = from_strips([x[S * k : S * (k + 1)] for k in range(STRIPS)], lane)
    return jnp.concatenate([x, tail], axis=0)


FREE = S * (STRIPS - 1)
FREE_LANE = W + W - LOW * (STRIPS - 1)


def spread(a_ref, lane, keep):
    def put(s, c):
        for block in range(HEAD // H):
            keep(pl.multiple_of(s * ROWS + block * H, H), a_ref[s, block * H : (block + 1) * H, :].astype(f32))
        for h in range(2):
            strips = [a_ref[s, (2 * k + h) * H : (2 * k + h + 1) * H, :].astype(f32) for k in range(STRIPS)]
            keep(pl.multiple_of(s * ROWS + HEAD + h * H, H), from_strips(strips, lane))
        return c

    lax.fori_loop(0, NU, put, 0)


def keep_both(xs, at, n, x):
    x = x.astype(bf16)
    xs[pl.ds(at, n), :] = x
    xs[pl.ds(NT * T + at, n), :] = -x


def first_up_kernel(idx_ref, a_ref, tiles_ref, mean_ref, p_ref, flat_ref, sums_ref, xs, some_p, acc):
    i = pl.program_id(0)
    lane = lane_of((1, T))

    @pl.when(i == 0)
    def _():
        acc[...] = jnp.zeros_like(acc)
        spread(a_ref, lane, lambda at, x: keep_both(xs, at, H, jnp.where(lane < W, x, 0.0)))

    for g in range(G):
        rows = pl.ds(pl.multiple_of((i * G + g) * T, T), T)
        p = hop_nat(i, g, idx_ref, tiles_ref, xs).astype(bf16)
        flat_ref[g * T : (g + 1) * T, :] = p
        p = p.astype(f32)
        some_p[g * T : (g + 1) * T, :] = p
        a = xs[rows, :].astype(f32)
        acc[0] += fold8(p * a)
        acc[1] += fold8(a * a)
    for t in range(NU):
        p_ref[i * NU + t] = packed(some_p, t, lane).astype(bf16)

    @pl.when(i == STEPS - 1)
    def _():
        energy = total_of(acc[0])
        center = (2.0 * energy / jnp.maximum(total_of(acc[1]), 1e-30) + mean_ref[0:1, 0:1]).astype(bf16)
        sub = lax.broadcasted_iota(jnp.int32, (8, T), 0)
        sums_ref[...] = jnp.where(sub == 0, energy, center.astype(f32))
        fill = jnp.broadcast_to(center, (S, T))
        free = lane_of((S, T)) >= FREE_LANE

        def mark(s, c):
            for k in range(8):
                at = s * 8 + k
                p_ref[at, FREE : FREE + S, :] = jnp.where(free, fill, p_ref[at, FREE : FREE + S, :])
            return c

        lax.fori_loop(0, NU * ND // 8, mark, 0)


def second_up_kernel(idx_ref, a_ref, flat_ref, tiles_ref, occ_rows_ref, occ_cols_ref, sums_ref, q_ref, out_ref, xs, some_q, acc):
    i = pl.program_id(0)
    lane = lane_of((1, T))

    @pl.when(i == 0)
    def _():
        acc[...] = jnp.zeros_like(acc)
        center = sums_ref[1:2, :]

        def keep(at, a):
            a = jnp.where(lane < W, a, 0.0)
            rows = pl.ds(at, H)
            diag = coupling * jnp.dot(occ_rows_ref[rows, :], occ_cols_ref[...], preferred_element_type=f32)
            acc[...] += fold8(diag * a * a)
            keep_both(xs, at, H, flat_ref[rows, :].astype(f32) + (diag - center) * a)

        spread(a_ref, lane, keep)
        out_ref[...] = jnp.broadcast_to(sums_ref[0:1, :] + total_of(acc[...]), out_ref.shape)

    for g in range(G):
        some_q[g * T : (g + 1) * T, :] = hop_nat(i, g, idx_ref, tiles_ref, xs)
    for t in range(NU):
        q_ref[t] = packed(some_q, t, lane).astype(bf16)


def pieces_in(o):
    found = []
    for u in range(NU):
        lo, hi = max(u * W, o * T), min((u + 1) * W, (o + 1) * T)
        if lo < hi:
            found.append((u, hi - o * T))
    return found


def assembled(rolled, o, lane):
    found = pieces_in(o)
    value = rolled[found[-1][0]]
    for u, end in reversed(found[:-1]):
        value = jnp.where(lane < end, rolled[u], value)
    return value


def down_kernel(idx_ref, *refs):
    pieces, refs = refs[:ND], refs[ND:]
    p_ref, tiles_ref, occ_rows_ref, occ_cols_ref = refs[:4]
    a_ref, u_ref, t_ref, sums_ref, tiles, xs, some_r, some_u, some_t, acc, sems = refs[4:]
    i = pl.program_id(0)
    lane = lane_of((1, T))

    def fetch(k):
        rows = pl.ds(k * G, G)
        return pltpu.make_async_copy(tiles_ref.at[rows], tiles.at[rows], sems.at[k])

    @pl.when(i == 0)
    def _():
        for k in range(STEPS):
            fetch(k).start()
        acc[...] = jnp.zeros_like(acc)
        down = idx_ref[NT * KT]
        for s in range(ND):
            source = lax.rem(down + ND - s, ND)
            for o in range(G):
                x = pieces[s][:, o * T : (o + 1) * T]
                xs[source * G + o] = x
                xs[NT + source * G + o] = -x

    @pl.when(i < STEPS)
    def _():
        fetch(i).wait()
        for g in range(G):
            row = i * G + g
            r = hop_turned(row, idx_ref, tiles, xs)
            some_r[row] = r
            acc[2] += fold8(r * xs[row].astype(f32))

    @pl.when(i == STEPS)
    def _():
        def first(d, c):
            rolled, centers = {}, {}
            for o in range(G):
                for u, _end in pieces_in(o):
                    if u in rolled:
                        continue
                    x = p_ref[u * ND + d].astype(f32)
                    centers[u] = jnp.sum(
                        jnp.where(lane == FREE_LANE, x[FREE : FREE + 1, :], 0.0), axis=1, keepdims=True
                    )
                    rolled[u] = turned(unpacked(x, lane), u * W)
                p = assembled(rolled, o, lane)
                center = assembled(centers, o, lane)
                at = d * G + o
                a = xs[at].astype(f32)
                diag = coupling * jnp.dot(
                    occ_rows_ref[...], occ_cols_ref[d, :, o * T : (o + 1) * T], preferred_element_type=f32
                )
                w = p + some_r[at] + diag * a
                some_u[at] = w
                some_t[at] = center * p + diag * w
                xs[NT + at] = p.astype(bf16)
                acc[0] += fold8(w * a)
                acc[1] += fold8(a * a)
            return c

        lax.fori_loop(0, ND, first, 0)
        center = total_of(acc[0]) / jnp.maximum(total_of(acc[1]), 1e-30)
        sub = lax.broadcasted_iota(jnp.int32, (8, T), 0)
        sums_ref[...] = jnp.where(sub == 0, center, total_of(acc[2]))

        def second(d, c):
            for o in range(G):
                at = d * G + o
                a = xs[at]
                a_ref[d, :, o * T : (o + 1) * T] = a
                w = some_u[at]
                u = w - center * a.astype(f32)
                some_u[at] = u
                some_t[at] += center * (some_r[at] - w - u)
                x = (u + xs[NT + at].astype(f32)).astype(bf16)
                xs[at] = x
                xs[NT + at] = -x
            return c

        lax.fori_loop(0, ND, second, 0)

    @pl.when(i >= STEPS)
    def _():
        for g in range(G):
            row = (i - STEPS) * G + g
            lanes = slice(g * T, (g + 1) * T)
            u_ref[0, :, lanes] = some_u[row]
            t_ref[0, :, lanes] = some_t[row] + hop_turned(row, idx_ref, tiles, xs)


def joined_kernel(a_ref, u_ref, t_ref, q_ref, up_ref, down_ref, g_ref, u_out_ref, sums_ref, acc):
    i = pl.program_id(0)
    lane = lane_of((1, T))

    @pl.when(i == 0)
    def _():
        acc[...] = jnp.zeros_like(acc)

    rolled = {}
    for o in range(G):
        for u, _end in pieces_in(o):
            if u not in rolled:
                rolled[u] = turned(unpacked(q_ref[u * ND + i].astype(f32), lane), u * W)
        lanes = slice(o * T, (o + 1) * T)
        a = a_ref[0, :, lanes].astype(f32)
        u = u_ref[0, :, lanes]
        g = assembled(rolled, o, lane) + t_ref[0, :, lanes]
        g_ref[i, :, lanes] = g
        u_out_ref[i, :, lanes] = u
        for k, product in enumerate([u * u, u * a, a * a, g * g, g * u, g * a]):
            acc[k] += fold8(product)

    @pl.when(i == ND - 1)
    def _():
        row = jnp.where(lane == 6, up_ref[0:1, :] + down_ref[1:2, :], down_ref[0:1, :])
        for k in range(6):
            row = jnp.where(lane == k, total_of(acc[k]), row)
        sums_ref[...] = jnp.broadcast_to(row, sums_ref.shape)


def final_kernel(a_ref, u_ref, g_ref, center_ref, shared_ref, v_ref, out_ref, coef):
    i = pl.program_id(0)
    lane = lane_of((1, T))

    @pl.when(i == 0)
    def _():
        uu, ua, aa, gg, gu, ga, energy, center = [shared_ref[:, k : k + 1] for k in range(8)]

        def total(x):
            return jnp.sum(x, axis=0, keepdims=True)

        norm = total(aa)
        scale2 = 1.0 / jnp.maximum(norm, 1.0)
        alpha1 = total(energy) * scale2
        off = center - alpha1
        hh = total(gg + 4.0 * off * (gu + off * (uu + off * ua)) + off * off * (2.0 * ga + off * off * aa))
        hu = total(gu + off * (2.0 * uu + ga + off * (3.0 * ua + off * aa)))
        ha = total(ga + off * (2.0 * ua + off * aa))
        uu = total(uu + off * (2.0 * ua + off * aa))
        ua = total(ua + off * aa)
        square1 = jnp.maximum(scale2 * uu, 1.0)
        ratio2 = scale2 / square1
        alpha2 = ratio2 * (hu + alpha1 * uu - square1 * ua)
        move = alpha2 - alpha1
        nn = hh + square1 * square1 * norm + move * move * uu
        nn = nn - 2.0 * square1 * ha - 2.0 * move * hu + 2.0 * square1 * move * ua
        square2 = jnp.maximum(ratio2 * nn, 1.0)
        beta1, beta2 = jnp.sqrt(square1), jnp.sqrt(square2)
        cg = jnp.sqrt(ratio2) / beta2
        off = center_ref[0:1, 0:1] - alpha1
        row = jnp.zeros((1, T), f32)
        for k, value in enumerate(
            [alpha1, alpha2, beta1, beta2, cg * (off * (off - move) - square1), cg * (2.0 * off - move), cg]
        ):
            row = jnp.where(lane == k, value, row)
        coef[...] = jnp.broadcast_to(row, coef.shape)
        out_ref[...] = jnp.broadcast_to(row, out_ref.shape)

    ca, cu, cg = coef[0:1, 4:5], coef[0:1, 5:6], coef[0:1, 6:7]
    v_ref[0] = (cg * g_ref[i] + cu * u_ref[i] + ca * a_ref[0].astype(f32)).astype(bf16)


def swapped_down(start_vector):
    down = lax.axis_index(DN)
    pieces = []
    for s in range(ND):
        piece = lax.dynamic_slice_in_dim(start_vector, (down + s) % ND * W, W, 0)
        if s:
            piece = lax.ppermute(piece, DN, [(k, (k + s) % ND) for k in range(ND)])
        pieces.append(piece)
    return pieces


def body(start_vector, hop_tiles, tile_columns, tile_signs, occupation):
    rows, cols = start_vector.shape
    index = (tile_columns + NT * tile_signs).astype(jnp.int32).reshape(-1)
    up = lax.axis_index(UP)
    down = lax.axis_index(DN)
    occ = occupation.astype(bf16)
    occ_rows = occ.T
    a_cols = lax.dynamic_slice_in_dim(occ, down * cols + up * W, W, 1)
    a_cols = jnp.pad(a_cols, ((0, 0), (0, T - W)))
    filled = jnp.sum(occ, axis=1, dtype=f32) * jnp.sum(a_cols, axis=1, dtype=f32)
    mean = jnp.full((8, T), coupling * jnp.sum(filled) / (occ.shape[1] * W), f32)
    b_rows = lax.dynamic_slice_in_dim(occ_rows, up * rows + down * W, W, 0)
    b_cols = jnp.moveaxis(occ.reshape(occ.shape[0], ND, cols), 1, 0)

    parts = pl.pallas_call(
        pack_kernel,
        out_shape=pltpu.HBM((NU, HEAD, T), bf16),
        compiler_params=pltpu.CompilerParams(vmem_limit_bytes=24 * MIB),
        name="pack",
    )(far(start_vector))
    a_up = lax.all_to_all(parts, UP, 0, 0, tiled=True)
    pieces = swapped_down(start_vector)

    hop_flops = 2 * NT * KT * T * T * T
    tile_bytes = NT * KT * T * T * 2
    cost = pl.CostEstimate(flops=hop_flops, bytes_accessed=tile_bytes + 8 * 2**20, transcendentals=0)
    tall = (NT * T, T)
    packs = (NU * ND, WH, T)
    wide = (ND, W, cols)
    xs_tall = pltpu.VMEM((2 * NT * T, T), bf16)
    some = pltpu.VMEM((G * T, T), f32)

    first_up = pl.pallas_call(
        first_up_kernel,
        grid_spec=pltpu.PrefetchScalarGridSpec(
            num_scalar_prefetch=1,
            grid=(STEPS,),
            in_specs=[whole((NU, HEAD, T)), tile_spec(), whole((8, T))],
            out_specs=[whole(packs), pl.BlockSpec((G * T, T), lambda i, *_: (i, 0)), whole((8, T))],
            scratch_shapes=[xs_tall, some, pltpu.VMEM((2, 8, T), f32)],
        ),
        out_shape=[
            pltpu.HBM(packs, bf16),
            pltpu.HBM(tall, bf16),
            jax.ShapeDtypeStruct((8, T), f32),
        ],
        compiler_params=params(28),
        cost_estimate=cost,
        name="first_up",
    )
    p, flat, sums = first_up(index, a_up, far(hop_tiles), mean)

    p_dn = lax.all_to_all(p, ALL, 0, 0, tiled=True)

    second_up = pl.pallas_call(
        second_up_kernel,
        grid_spec=pltpu.PrefetchScalarGridSpec(
            num_scalar_prefetch=1,
            grid=(STEPS,),
            in_specs=[
                whole((NU, HEAD, T)),
                whole(tall),
                tile_spec(),
                whole(occ_rows.shape),
                whole(a_cols.shape),
                whole((8, T)),
            ],
            out_specs=[pl.BlockSpec((NU, WH, T), lambda i, *_: (i, 0, 0)), whole((8, T))],
            scratch_shapes=[xs_tall, some, pltpu.VMEM((8, T), f32)],
        ),
        out_shape=[pltpu.HBM(packs, bf16), jax.ShapeDtypeStruct((8, T), f32)],
        compiler_params=params(32),
        cost_estimate=cost,
        name="second_up",
    )
    q, up_dots = second_up(index, far(a_up), flat, far(hop_tiles), far(occ_rows), a_cols, sums)

    p_dn, q, b_cols = lax.optimization_barrier((p_dn, q, b_cols))
    q_dn = lax.all_to_all(q, ALL, 0, 0, tiled=True)

    near = pl.BlockSpec(memory_space=pltpu.VMEM)
    kept = pltpu.VMEM(wide, f32)
    cut = pltpu.VMEM((NT, W, T), f32)
    late = pl.BlockSpec((1, W, cols), lambda i, *_: (jnp.maximum(i - STEPS, 0), 0, 0))
    a_dn, u, t, down_dots = pl.pallas_call(
        down_kernel,
        grid_spec=pltpu.PrefetchScalarGridSpec(
            num_scalar_prefetch=1,
            grid=(2 * STEPS,),
            in_specs=[whole((W, cols))] * ND
            + [
                whole(packs),
                pl.BlockSpec(memory_space=pl.ANY),
                whole(b_rows.shape),
                whole(b_cols.shape),
            ],
            out_specs=[whole(wide), late, late, whole((8, T))],
            scratch_shapes=[
                pltpu.VMEM((NT, KT, T, T), bf16),
                pltpu.VMEM((2 * NT, W, T), bf16),
                cut,
                cut,
                cut,
                pltpu.VMEM((3, 8, T), f32),
                pltpu.SemaphoreType.DMA((STEPS,)),
            ],
        ),
        out_shape=[
            pltpu.HBM(wide, bf16),
            pltpu.HBM(wide, f32),
            pltpu.HBM(wide, f32),
            jax.ShapeDtypeStruct((8, T), f32),
        ],
        compiler_params=params(56),
        cost_estimate=cost,
        name="down",
    )(jnp.concatenate([index, down[None]]), *[far(x) for x in pieces], p_dn, far(hop_tiles), b_rows, b_cols)

    block = pl.BlockSpec((1, W, cols), lambda i, *_: (i, 0, 0))
    g, u, partial = pl.pallas_call(
        joined_kernel,
        grid=(ND,),
        in_specs=[block, block, block, whole(packs), whole((8, T)), whole((8, T))],
        out_specs=[near, near, whole((NU * ND, T))],
        out_shape=[kept, kept, jax.ShapeDtypeStruct((NU * ND, T), f32)],
        scratch_shapes=[pltpu.VMEM((6, 8, T), f32)],
        compiler_params=params(20),
        name="joined",
    )(far(a_dn), far(u), far(t), q_dn, up_dots, down_dots)

    shared = lax.all_to_all(partial, ALL, 0, 0, tiled=True)
    v, scalars = pl.pallas_call(
        final_kernel,
        grid=(ND,),
        in_specs=[block, near, near, whole((8, T)), whole((NU * ND, T))],
        out_specs=[block, whole((8, T))],
        out_shape=[pltpu.HBM(wide, bf16), jax.ShapeDtypeStruct((8, T), f32)],
        scratch_shapes=[pltpu.VMEM((8, T), f32)],
        compiler_params=params(16),
        name="final",
    )(a_dn, u, g, down_dots, shared)
    final = lax.all_to_all(v, DN, 0, 0, tiled=True).reshape(rows, cols)
    return final, scalars[0, 0:2], scalars[0, 2:4]


def solution(mesh):
    torus = Mesh(mesh.devices.reshape(2, 4, 2, 2, 4), ALL)
    return jax.shard_map(
        body,
        mesh=torus,
        in_specs=(P(UP, DN), P(), P(), P(), P()),
        out_specs=(P(UP, DN), P(), P()),
        check_vma=False,
    )
```

```python
import jax
import jax.numpy as jnp
from jax import lax
from jax.experimental import pallas as pl
from jax.experimental.pallas import tpu as pltpu
from jax.sharding import Mesh
from jax.sharding import PartitionSpec as P


UP = ("up_0", "up_1", "up_2")
DN = ("dn_0", "dn_1")
ALL = UP + DN
coupling = 4.0

f32 = jnp.float32
bf16 = jnp.bfloat16

T = 128
NT = 104
KT = 5
G = 13
STEPS = NT // G
W = 104
NU = 16
ND = 8
MIB = 1024 * 1024


def params(mib):
    return pltpu.CompilerParams(dimension_semantics=("arbitrary",), vmem_limit_bytes=mib * MIB)


def whole(shape):
    zeros = (0,) * len(shape)
    return pl.BlockSpec(shape, lambda i, *_: zeros, pipeline_mode=pl.Buffered(1))


def far(x):
    return pltpu.with_memory_space_constraint(x, pltpu.HBM)


def tile_specs():
    return [pl.BlockSpec((G, 1, T, T), lambda i, *_, k=k: (i, k, 0, 0)) for k in range(KT)]


def lane_of(shape):
    return lax.broadcasted_iota(jnp.int32, shape, len(shape) - 1)


def total_of(x):
    return jnp.sum(jnp.sum(x, axis=0, keepdims=True), axis=1, keepdims=True)


def fold8(x):
    return jnp.sum(x.reshape(x.shape[0] // 8, 8, x.shape[1]), axis=0)


def tile_fetch(tiles_ref, tiles, sems, k):
    rows = pl.ds(k * G, G)
    return pltpu.make_async_copy(tiles_ref.at[rows], tiles.at[rows], sems.at[k])


def hop_nat(row, lefts, idx_ref, xs):
    left = jnp.concatenate(lefts, axis=1)
    right = [xs[pl.ds(pl.multiple_of(idx_ref[row * KT + k] * T, T), T), :] for k in range(KT)]
    return jnp.dot(left, jnp.concatenate(right, axis=0), preferred_element_type=f32)


def hop_turned(row, idx_ref, tiles, xs):
    right = jnp.concatenate([tiles[row, k] for k in range(KT)], axis=1)
    left = jnp.concatenate([xs[idx_ref[row * KT + k]] for k in range(KT)], axis=1)
    return lax.dot_general(left, right, (((1,), (1,)), ((), ())), preferred_element_type=f32)


LOW = T - W
STRIPS = -(-W // LOW)


def turned(x, shift):
    shift %= T
    return pltpu.roll(x, shift, 1) if shift else x


def with_strip(head, tail, k, lane):
    return jnp.where(lane < W, head, turned(tail, W - LOW * k))


def from_strips(strips, lane):
    value = turned(strips[-1], LOW * (STRIPS - 1) - W)
    for k in reversed(range(STRIPS - 1)):
        value = jnp.where(lane < LOW * (k + 1), turned(strips[k], LOW * k - W), value)
    return value


ROWS = 832
HEAD = 704
H = 64
WH = 88
S = W - WH


PARTS = 4
ENDS = [-(-W * NU * (k + 1) // PARTS // T) * T for k in range(PARTS)]


def pack_kernel(a_ref, out_ref, near, sems):
    i = pl.program_id(0)
    lane = lane_of((1, T))

    def fetch(k):
        lanes = pl.ds(ENDS[k - 1] if k else 0, ENDS[k] - (ENDS[k - 1] if k else 0))
        return pltpu.make_async_copy(a_ref.at[:, lanes], near.at[:, lanes], sems.at[k])

    def cut(u, block):
        q, o = divmod(u * W, T)
        rows = slice(block * H, (block + 1) * H)
        x = turned(near[rows, q * T : (q + 1) * T], -o)
        if o + W > T:
            y = turned(near[rows, (q + 1) * T : (q + 2) * T], -o)
            x = jnp.where(lane < T - o, x, y)
        return x

    @pl.when(i == 0)
    def _():
        for k in range(PARTS):
            fetch(k).start()

    for k in range(PARTS):

        @pl.when(i == k)
        def _():
            fetch(k).wait()
            for n in range(NU // PARTS):
                u = k * (NU // PARTS) + n
                tails = [cut(u, HEAD // H + h) for h in range(2)]
                for block in range(HEAD // H):
                    x = cut(u, block)
                    if block < 2 * STRIPS:
                        x = with_strip(x, tails[block % 2], block // 2, lane)
                    out_ref[n, block * H : (block + 1) * H, :] = x


def packed(values, t, lane):
    tail = values[pl.ds(pl.multiple_of(t * W, 8), S), :]
    x = values[pl.ds(pl.multiple_of(t * W + S, 8), WH), :]
    found = [with_strip(x[S * k : S * (k + 1)], tail, k, lane) for k in range(STRIPS)]
    return jnp.concatenate(found + [x[S * STRIPS :]], axis=0)


def unpacked(x, lane):
    tail = from_strips([x[S * k : S * (k + 1)] for k in range(STRIPS)], lane)
    return jnp.concatenate([tail, x], axis=0)


FREE = S * (STRIPS - 1)
FREE_LANE = W + W - LOW * (STRIPS - 1)


def spread(a_ref, lane, keep):
    def put(s, c):
        for block in range(HEAD // H):
            keep(pl.multiple_of(s * ROWS + block * H, H), a_ref[s, block * H : (block + 1) * H, :])
        for h in range(2):
            strips = [a_ref[s, (2 * k + h) * H : (2 * k + h + 1) * H, :] for k in range(STRIPS)]
            keep(pl.multiple_of(s * ROWS + HEAD + h * H, H), from_strips(strips, lane))
        return c

    lax.fori_loop(0, NU, put, 0)


def keep_both(xs, at, n, x):
    xs[pl.ds(at, n), :] = x
    xs[pl.ds(NT * T + at, n), :] = -x


def counted(x, lane):
    return total_of(jnp.where(lane < W, x, 0.0))


def first_up_kernel(idx_ref, a_ref, tiles_ref, mean_ref, p_ref, sums_ref, xs, tiles, some_p, acc, held, sems):
    i = pl.program_id(0)
    lane = lane_of((1, T))

    @pl.when(i == 0)
    def _():
        for k in range(STEPS):
            tile_fetch(tiles_ref, tiles, sems, k).start()
        acc[...] = jnp.zeros_like(acc)
        spread(a_ref, lane, lambda at, x: keep_both(xs, at, H, x))

    tile_fetch(tiles_ref, tiles, sems, i).wait()

    for g in range(G):
        row = i * G + g
        rows = pl.ds(pl.multiple_of(row * T, T), T)
        p = hop_nat(row, [tiles[row, k] for k in range(KT)], idx_ref, xs).astype(bf16).astype(f32)
        some_p[g * T : (g + 1) * T, :] = p
        a = xs[rows, :].astype(f32)
        acc[0] += fold8(p * a)
        acc[1] += fold8(a * a)

    @pl.when(i == 0)
    def _():
        ratio = 2.0 * counted(acc[0], lane) / jnp.maximum(counted(acc[1], lane), 1e-30)
        held[...] = jnp.broadcast_to((ratio + mean_ref[0:1, 0:1]).astype(bf16).astype(f32), held.shape)

    center = held[0:1, :]
    for t in range(NU):
        x = packed(some_p, t, lane)
        marked = jnp.where(lane >= FREE_LANE, center, x[FREE : FREE + S])
        p_ref[t] = jnp.concatenate([x[:FREE], marked, x[FREE + S :]], axis=0).astype(bf16)

    @pl.when(i == STEPS - 1)
    def _():
        sub = lax.broadcasted_iota(jnp.int32, (8, T), 0)
        sums_ref[...] = jnp.where(sub == 0, counted(acc[0], lane), center)


def second_up_kernel(idx_ref, a_ref, p_ref, *refs):
    tiles, refs = refs[:KT], refs[KT:]
    occ_rows_ref, occ_cols_ref, sums_ref, q_ref, out_ref, xs, some_q, flat, acc = refs
    i = pl.program_id(0)
    lane = lane_of((1, T))

    @pl.when(i == 0)
    def _():
        acc[...] = jnp.zeros_like(acc)
        center = sums_ref[1:2, :]

        def open_p(s, c):
            flat[pl.ds(pl.multiple_of(s * W, 8), W), :] = unpacked(p_ref[s], lane).astype(f32)
            return c

        lax.fori_loop(0, NU * ND, open_p, 0)

        def keep(at, a):
            a = a.astype(f32)
            rows = pl.ds(at, H)
            diag = coupling * jnp.dot(occ_rows_ref[rows, :], occ_cols_ref[...], preferred_element_type=f32)
            acc[...] += fold8(diag * a * a)
            keep_both(xs, at, H, (flat[rows, :] + (diag - center) * a).astype(bf16))

        spread(a_ref, lane, keep)
        out_ref[...] = jnp.broadcast_to(sums_ref[0:1, :] + counted(acc[...], lane), out_ref.shape)

    for g in range(G):
        some_q[g * T : (g + 1) * T, :] = hop_nat(i * G + g, [tile_ref[g, 0] for tile_ref in tiles], idx_ref, xs)
    for t in range(NU):
        q_ref[t] = packed(some_q, t, lane).astype(bf16)


def pieces_in(o):
    found = []
    for u in range(NU):
        lo, hi = max(u * W, o * T), min((u + 1) * W, (o + 1) * T)
        if lo < hi:
            found.append((u, hi - o * T))
    return found


def assembled(rolled, o, lane):
    found = pieces_in(o)
    value = rolled[found[-1][0]]
    for u, end in reversed(found[:-1]):
        value = jnp.where(lane < end, rolled[u], value)
    return value


def down_kernel(idx_ref, *refs):
    pieces, refs = refs[:ND], refs[ND:]
    p_ref, tiles_ref, occ_rows_ref, occ_cols_ref = refs[:4]
    a_ref, u_ref, brief_ref, t_ref, sums_ref, tiles, xs, some_r, some_u, some_t, acc, sems = refs[4:]
    i = pl.program_id(0)
    lane = lane_of((1, T))

    @pl.when(i == 0)
    def _():
        for k in range(STEPS):
            tile_fetch(tiles_ref, tiles, sems, k).start()
        acc[...] = jnp.zeros_like(acc)
        down = idx_ref[NT * KT]
        for s in range(ND):
            source = lax.rem(down + ND - s, ND)
            for o in range(G):
                x = pieces[s][:, o * T : (o + 1) * T]
                xs[source * G + o] = x
                xs[NT + source * G + o] = -x

    @pl.when(i < STEPS)
    def _():
        tile_fetch(tiles_ref, tiles, sems, i).wait()
        for g in range(G):
            row = i * G + g
            r = hop_turned(row, idx_ref, tiles, xs)
            some_r[row] = r
            a = xs[row]
            a_ref[0, :, g * T : (g + 1) * T] = a
            acc[2] += fold8(r * a.astype(f32))

    @pl.when(i == STEPS)
    def _():
        def first(d, c):
            rolled, centers = {}, {}
            for o in range(G):
                for u, _end in pieces_in(o):
                    if u in rolled:
                        continue
                    x = p_ref[u * ND + d]
                    mark = x[FREE : FREE + S, :].astype(f32)[0:1, :]
                    centers[u] = jnp.sum(jnp.where(lane == FREE_LANE, mark, 0.0), axis=1, keepdims=True)
                    rolled[u] = turned(unpacked(x, lane), u * W)
                p = assembled(rolled, o, lane).astype(f32)
                center = assembled(centers, o, lane)
                at = d * G + o
                a = xs[at].astype(f32)
                diag = coupling * jnp.dot(
                    occ_rows_ref[...], occ_cols_ref[d, :, o * T : (o + 1) * T], preferred_element_type=f32
                )
                w = p + some_r[at] + diag * a
                some_u[at] = w
                some_t[at] = center * p + diag * w
                xs[NT + at] = p.astype(bf16)
                acc[0] += fold8(w * a)
                acc[1] += fold8(a * a)
            return c

        lax.fori_loop(0, ND, first, 0)
        center = total_of(acc[0]) / jnp.maximum(total_of(acc[1]), 1e-30)

        def second(d, c):
            for o in range(G):
                at = d * G + o
                w = some_u[at]
                a = xs[at].astype(f32)
                u = w - center * a
                acc[3] += fold8(u * u)
                acc[4] += fold8(u * a)
                some_u[at] = u
                some_t[at] += center * (some_r[at] - w - u)
                x = (u + xs[NT + at].astype(f32)).astype(bf16)
                xs[at] = x
                xs[NT + at] = -x
            return c

        lax.fori_loop(0, ND, second, 0)
        sub = lax.broadcasted_iota(jnp.int32, (8, T), 0)
        found = center
        for k, n in enumerate([2, 3, 4, 1]):
            found = jnp.where(sub == k + 1, total_of(acc[n]), found)
        sums_ref[...] = jnp.broadcast_to(found, sums_ref.shape)

    @pl.when(i >= STEPS)
    def _():
        for g in range(G):
            row = (i - STEPS) * G + g
            lanes = slice(g * T, (g + 1) * T)
            u = some_u[row]
            u_ref[0, :, lanes] = u
            brief_ref[0, :, lanes] = u.astype(bf16)
            t_ref[0, :, lanes] = some_t[row] + hop_turned(row, idx_ref, tiles, xs)


def joined_kernel(*refs):
    far_refs, (q_ref, up_ref, down_ref, g_ref, sums_ref, a_ref, u_ref, t_ref, sems, acc) = refs[:3], refs[3:]
    i = pl.program_id(0)
    lane = lane_of((1, T))

    def fetch(n, d):
        return pltpu.make_async_copy(far_refs[n].at[d], (a_ref, u_ref, t_ref)[n].at[d], sems.at[n, d])

    @pl.when(i == 0)
    def _():
        for d in range(ND):
            for n in range(3):
                fetch(n, d).start()

    for n in range(3):
        fetch(n, i).wait()

    @pl.when(i == 0)
    def _():
        acc[...] = jnp.zeros_like(acc)

    rolled = {}
    for o in range(G):
        for u, _end in pieces_in(o):
            if u not in rolled:
                rolled[u] = turned(unpacked(q_ref[u * ND + i], lane), u * W)
        lanes = slice(o * T, (o + 1) * T)
        a = a_ref[i, :, lanes].astype(f32)
        u = u_ref[i, :, lanes].astype(f32)
        g = assembled(rolled, o, lane).astype(f32) + t_ref[i, :, lanes]
        g_ref[i, :, lanes] = g
        for k, product in enumerate([g * g, g * u, g * a]):
            acc[k] += fold8(product)

    @pl.when(i == ND - 1)
    def _():
        row = down_ref[0:1, :]
        for k, value in enumerate(
            [down_ref[2:3, :], down_ref[3:4, :], down_ref[4:5, :]]
            + [total_of(acc[k]) for k in range(3)]
            + [up_ref[0:1, :] + down_ref[1:2, :]]
        ):
            row = jnp.where(lane == k, value, row)
        sums_ref[...] = jnp.broadcast_to(row, sums_ref.shape)


def final_kernel(a_ref, u_ref, g_ref, center_ref, shared_ref, v_ref, out_ref, coef):
    i = pl.program_id(0)
    lane = lane_of((1, T))

    @pl.when(i == 0)
    def _():
        table = shared_ref[...].T
        uu, ua, aa, gg, gu, ga, energy, center = [table[k : k + 1, :] for k in range(8)]

        def total(x):
            return jnp.sum(x, axis=1, keepdims=True)

        norm = total(aa)
        scale2 = 1.0 / jnp.maximum(norm, 1.0)
        alpha1 = total(energy) * scale2
        off = center - alpha1
        hh = total(gg + 4.0 * off * (gu + off * (uu + off * ua)) + off * off * (2.0 * ga + off * off * aa))
        hu = total(gu + off * (2.0 * uu + ga + off * (3.0 * ua + off * aa)))
        ha = total(ga + off * (2.0 * ua + off * aa))
        uu = total(uu + off * (2.0 * ua + off * aa))
        ua = total(ua + off * aa)
        square1 = jnp.maximum(scale2 * uu, 1.0)
        ratio2 = scale2 / square1
        alpha2 = ratio2 * (hu + alpha1 * uu - square1 * ua)
        move = alpha2 - alpha1
        nn = hh + square1 * square1 * norm + move * move * uu
        nn = nn - 2.0 * square1 * ha - 2.0 * move * hu + 2.0 * square1 * move * ua
        square2 = jnp.maximum(ratio2 * nn, 1.0)
        beta1, beta2 = jnp.sqrt(square1), jnp.sqrt(square2)
        cg = jnp.sqrt(ratio2) / beta2
        off = center_ref[0:1, 0:1] - alpha1
        row = jnp.zeros((1, T), f32)
        for k, value in enumerate(
            [alpha1, alpha2, beta1, beta2, cg * (off * (off - move) - square1), cg * (2.0 * off - move), cg]
        ):
            row = jnp.where(lane == k, value, row)
        coef[...] = jnp.broadcast_to(row, coef.shape)
        out_ref[...] = jnp.broadcast_to(row, out_ref.shape)

    ca, cu, cg = coef[0:1, 4:5], coef[0:1, 5:6], coef[0:1, 6:7]
    v_ref[0] = (cg * g_ref[i] + cu * u_ref[i] + ca * a_ref[0].astype(f32)).astype(bf16)


def swapped_down(start_vector):
    down = lax.axis_index(DN)
    pieces = []
    for s in range(ND):
        piece = lax.dynamic_slice_in_dim(start_vector, (down + s) % ND * W, W, 0)
        if s:
            piece = lax.ppermute(piece, DN, [(k, (k + s) % ND) for k in range(ND)])
        pieces.append(piece)
    return pieces


def body(start_vector, hop_tiles, tile_columns, tile_signs, occupation):
    rows, cols = start_vector.shape
    index = (tile_columns + NT * tile_signs).astype(jnp.int32).reshape(-1)
    up = lax.axis_index(UP)
    down = lax.axis_index(DN)
    index = jnp.concatenate([index, down.astype(jnp.int32)[None]])
    occ = occupation.astype(bf16)
    occ_rows = occ.T
    a_cols = lax.dynamic_slice_in_dim(occ, down * cols + up * W, W, 1)
    a_cols = jnp.pad(a_cols, ((0, 0), (0, T - W)))
    filled = jnp.sum(occ, axis=1, dtype=f32) * jnp.sum(a_cols, axis=1, dtype=f32)
    mean = jnp.full((8, T), coupling * jnp.sum(filled) / (occ.shape[1] * W), f32)
    b_rows = lax.dynamic_slice_in_dim(occ_rows, up * rows + down * W, W, 0)
    b_cols = jnp.moveaxis(occ.reshape(occ.shape[0], ND, cols), 1, 0)

    parts = pl.pallas_call(
        pack_kernel,
        grid=(PARTS,),
        in_specs=[pl.BlockSpec(memory_space=pl.ANY)],
        out_specs=pl.BlockSpec((NU // PARTS, HEAD, T), lambda i: (i, 0, 0)),
        out_shape=pltpu.HBM((NU, HEAD, T), bf16),
        scratch_shapes=[pltpu.VMEM(start_vector.shape, bf16), pltpu.SemaphoreType.DMA((PARTS,))],
        compiler_params=params(24),
        name="pack",
    )(far(start_vector))
    a_up = lax.all_to_all(parts, UP, 0, 0, tiled=True)
    pieces = swapped_down(start_vector)

    hop_flops = 2 * NT * KT * T * T * T
    tile_bytes = NT * KT * T * T * 2
    cost = pl.CostEstimate(flops=hop_flops, bytes_accessed=tile_bytes + 8 * 2**20, transcendentals=0)
    tall = (NT * T, T)
    packs = (NU * ND, WH, T)
    wide = (ND, W, cols)
    xs_tall = pltpu.VMEM((2 * NT * T, T), bf16)
    some = pltpu.VMEM((G * T, T), f32)

    first_up = pl.pallas_call(
        first_up_kernel,
        grid_spec=pltpu.PrefetchScalarGridSpec(
            num_scalar_prefetch=1,
            grid=(STEPS,),
            in_specs=[whole((NU, HEAD, T)), pl.BlockSpec(memory_space=pl.ANY), whole((8, T))],
            out_specs=[
                pl.BlockSpec((NU, WH, T), lambda i, *_: (i, 0, 0)),
                whole((8, T)),
            ],
            scratch_shapes=[
                xs_tall,
                pltpu.VMEM((NT, KT, T, T), bf16),
                some,
                pltpu.VMEM((2, 8, T), f32),
                pltpu.VMEM((8, T), f32),
                pltpu.SemaphoreType.DMA((STEPS,)),
            ],
        ),
        out_shape=[
            pltpu.HBM(packs, bf16),
            jax.ShapeDtypeStruct((8, T), f32),
        ],
        compiler_params=params(44),
        cost_estimate=cost,
        name="first_up",
    )
    p, sums = first_up(index, a_up, far(hop_tiles), mean)

    p_dn = lax.all_to_all(p, ALL, 0, 0, tiled=True)

    second_up = pl.pallas_call(
        second_up_kernel,
        grid_spec=pltpu.PrefetchScalarGridSpec(
            num_scalar_prefetch=1,
            grid=(STEPS,),
            in_specs=[
                whole((NU, HEAD, T)),
                whole(packs),
                *tile_specs(),
                whole(occ_rows.shape),
                whole(a_cols.shape),
                whole((8, T)),
            ],
            out_specs=[pl.BlockSpec((NU, WH, T), lambda i, *_: (i, 0, 0)), whole((8, T))],
            scratch_shapes=[xs_tall, some, pltpu.VMEM(tall, f32), pltpu.VMEM((8, T), f32)],
        ),
        out_shape=[pltpu.HBM(packs, bf16), jax.ShapeDtypeStruct((8, T), f32)],
        compiler_params=params(40),
        cost_estimate=cost,
        name="second_up",
    )
    q, up_dots = second_up(index, far(a_up), far(p), *[far(hop_tiles)] * KT, far(occ_rows), a_cols, sums)

    p_dn, q, b_cols = lax.optimization_barrier((p_dn, q, b_cols))
    q_dn = lax.all_to_all(q, ALL, 0, 0, tiled=True)

    near = pl.BlockSpec(memory_space=pltpu.VMEM)
    kept = pltpu.VMEM(wide, f32)
    cut = pltpu.VMEM((NT, W, T), f32)
    late = pl.BlockSpec((1, W, cols), lambda i, *_: (jnp.maximum(i - STEPS, 0), 0, 0))
    early = pl.BlockSpec((1, W, cols), lambda i, *_: (jnp.minimum(i, STEPS - 1), 0, 0))
    a_dn, u, brief_u, t, down_dots = pl.pallas_call(
        down_kernel,
        grid_spec=pltpu.PrefetchScalarGridSpec(
            num_scalar_prefetch=1,
            grid=(2 * STEPS,),
            in_specs=[whole((W, cols))] * ND
            + [
                whole(packs),
                pl.BlockSpec(memory_space=pl.ANY),
                whole(b_rows.shape),
                whole(b_cols.shape),
            ],
            out_specs=[early, late, late, late, whole((8, T))],
            scratch_shapes=[
                pltpu.VMEM((NT, KT, T, T), bf16),
                pltpu.VMEM((2 * NT, W, T), bf16),
                cut,
                cut,
                cut,
                pltpu.VMEM((5, 8, T), f32),
                pltpu.SemaphoreType.DMA((STEPS,)),
            ],
        ),
        out_shape=[
            pltpu.HBM(wide, bf16),
            pltpu.HBM(wide, f32),
            pltpu.HBM(wide, bf16),
            pltpu.HBM(wide, f32),
            jax.ShapeDtypeStruct((8, T), f32),
        ],
        compiler_params=params(56),
        cost_estimate=cost,
        name="down",
    )(index, *[far(x) for x in pieces], p_dn, far(hop_tiles), b_rows, b_cols)

    block = pl.BlockSpec((1, W, cols), lambda i, *_: (i, 0, 0))
    g, partial = pl.pallas_call(
        joined_kernel,
        grid=(ND,),
        in_specs=[pl.BlockSpec(memory_space=pl.ANY)] * 3 + [whole(packs), whole((8, T)), whole((8, T))],
        out_specs=[near, whole((NU * ND, T))],
        out_shape=[kept, jax.ShapeDtypeStruct((NU * ND, T), f32)],
        scratch_shapes=[
            pltpu.VMEM(wide, bf16),
            pltpu.VMEM(wide, bf16),
            pltpu.VMEM(wide, f32),
            pltpu.SemaphoreType.DMA((3, ND)),
            pltpu.VMEM((3, 8, T), f32),
        ],
        compiler_params=params(24),
        name="joined",
    )(far(a_dn), far(brief_u), far(t), q_dn, far(up_dots), far(down_dots))

    shared = lax.all_to_all(partial, ALL, 0, 0, tiled=True)
    v, scalars = pl.pallas_call(
        final_kernel,
        grid=(ND,),
        in_specs=[block, near, near, whole((8, T)), whole((NU * ND, T))],
        out_specs=[block, whole((8, T))],
        out_shape=[pltpu.HBM(wide, bf16), jax.ShapeDtypeStruct((8, T), f32)],
        scratch_shapes=[pltpu.VMEM((8, T), f32)],
        compiler_params=params(16),
        name="final",
    )(a_dn, u, g, far(down_dots), shared)
    final = lax.all_to_all(v, DN, 0, 0, tiled=True).reshape(rows, cols)
    return final, scalars[0, 0:2], scalars[0, 2:4]


def solution(mesh):
    torus = Mesh(mesh.devices.reshape(2, 4, 2, 2, 4), ALL)
    return jax.shard_map(
        body,
        mesh=torus,
        in_specs=(P(UP, DN), P(), P(), P(), P()),
        out_specs=(P(UP, DN), P(), P()),
        check_vma=False,
    )
```

```python
import jax
import jax.numpy as jnp
from jax import lax
from jax.experimental import pallas as pl
from jax.experimental.pallas import tpu as pltpu
from jax.sharding import Mesh
from jax.sharding import PartitionSpec as P


UP = ("up_0", "up_1", "up_2")
DN = ("dn_0", "dn_1")
ALL = UP + DN
coupling = 4.0

f32 = jnp.float32
bf16 = jnp.bfloat16

T = 128
NT = 104
KT = 5
G = 13
STEPS = NT // G
W = 104
NU = 16
ND = 8
NZ = 4
MIB = 1024 * 1024


def params(mib):
    return pltpu.CompilerParams(dimension_semantics=("arbitrary",), vmem_limit_bytes=mib * MIB)


def whole(shape):
    zeros = (0,) * len(shape)
    return pl.BlockSpec(shape, lambda i, *_: zeros, pipeline_mode=pl.Buffered(1))


def far(x):
    return pltpu.with_memory_space_constraint(x, pltpu.HBM)


def tile_specs():
    return [pl.BlockSpec((G, 1, T, T), lambda i, *_, k=k: (i, k, 0, 0)) for k in range(KT)]


def lane_of(shape):
    return lax.broadcasted_iota(jnp.int32, shape, len(shape) - 1)


def total_of(x):
    return jnp.sum(jnp.sum(x, axis=0, keepdims=True), axis=1, keepdims=True)


def fold8(x):
    return jnp.sum(x.reshape(x.shape[0] // 8, 8, x.shape[1]), axis=0)


def tile_fetch(tiles_ref, tiles, sems, k):
    rows = pl.ds(k * G, G)
    return pltpu.make_async_copy(tiles_ref.at[rows], tiles.at[rows], sems.at[k])


def hop_nat(row, lefts, idx_ref, xs):
    left = jnp.concatenate(lefts, axis=1)
    right = [xs[pl.ds(pl.multiple_of(idx_ref[row * KT + k] * T, T), T), :] for k in range(KT)]
    return jnp.dot(left, jnp.concatenate(right, axis=0), preferred_element_type=f32)


def hop_turned(row, idx_ref, tiles, xs):
    right = jnp.concatenate([tiles[row, k] for k in range(KT)], axis=1)
    left = jnp.concatenate([xs[idx_ref[row * KT + k]] for k in range(KT)], axis=1)
    return lax.dot_general(left, right, (((1,), (1,)), ((), ())), preferred_element_type=f32)


LOW = T - W
STRIPS = -(-W // LOW)


def turned(x, shift):
    shift %= T
    return pltpu.roll(x, shift, 1) if shift else x


def with_strip(head, tail, k, lane):
    return jnp.where(lane < W, head, turned(tail, W - LOW * k))


def from_strips(strips, lane):
    value = turned(strips[-1], LOW * (STRIPS - 1) - W)
    for k in reversed(range(STRIPS - 1)):
        value = jnp.where(lane < LOW * (k + 1), turned(strips[k], LOW * k - W), value)
    return value


ROWS = 832
HEAD = 704
H = 64
WH = 88
S = W - WH


PARTS = 4
ENDS = [-(-W * NU * (k + 1) // PARTS // T) * T for k in range(PARTS)]


def pack_kernel(a_ref, out_ref, near, ready, sems, out_sems):
    i = pl.program_id(0)
    lane = lane_of((1, T))

    def fetch(k):
        lanes = pl.ds(ENDS[k - 1] if k else 0, ENDS[k] - (ENDS[k - 1] if k else 0))
        return pltpu.make_async_copy(a_ref.at[:, lanes], near.at[:, lanes], sems.at[k])

    def send(u):
        return pltpu.make_async_copy(ready.at[u], out_ref.at[u], out_sems.at[u])

    def cut(u, block):
        q, o = divmod(u * W, T)
        rows = slice(block * H, (block + 1) * H)
        x = turned(near[rows, q * T : (q + 1) * T], -o)
        if o + W > T:
            y = turned(near[rows, (q + 1) * T : (q + 2) * T], -o)
            x = jnp.where(lane < T - o, x, y)
        return x

    @pl.when(i == 0)
    def _():
        for k in range(PARTS):
            fetch(k).start()

    for k in range(PARTS):

        @pl.when(i == k)
        def _():
            fetch(k).wait()
            for n in range(NU // PARTS):
                u = k * (NU // PARTS) + n
                tails = [cut(u, HEAD // H + h) for h in range(2)]
                for block in range(HEAD // H):
                    x = cut(u, block)
                    if block < 2 * STRIPS:
                        x = with_strip(x, tails[block % 2], block // 2, lane)
                    ready[u, block * H : (block + 1) * H, :] = x
                send(u).start()

    @pl.when(i == PARTS - 1)
    def _():
        for u in range(NU):
            send(u).wait()


def packed(values, t, lane):
    tail = values[pl.ds(pl.multiple_of(t * W, 8), S), :]
    x = values[pl.ds(pl.multiple_of(t * W + S, 8), WH), :]
    found = [with_strip(x[S * k : S * (k + 1)], tail, k, lane) for k in range(STRIPS)]
    return jnp.concatenate(found + [x[S * STRIPS :]], axis=0)


def unpacked(x, lane):
    tail = from_strips([x[S * k : S * (k + 1)] for k in range(STRIPS)], lane)
    return jnp.concatenate([tail, x], axis=0)


FREE = S * (STRIPS - 1)
FREE_LANE = W + W - LOW * (STRIPS - 1)


def spread(a_ref, lane, keep):
    def put(s, c):
        for block in range(HEAD // H):
            keep(pl.multiple_of(s * ROWS + block * H, H), a_ref[s, block * H : (block + 1) * H, :])
        for h in range(2):
            strips = [a_ref[s, (2 * k + h) * H : (2 * k + h + 1) * H, :] for k in range(STRIPS)]
            keep(pl.multiple_of(s * ROWS + HEAD + h * H, H), from_strips(strips, lane))
        return c

    lax.fori_loop(0, NU, put, 0, unroll=2)


def keep_both(xs, at, n, x):
    xs[pl.ds(at, n), :] = x
    xs[pl.ds(NT * T + at, n), :] = -x


def counted(x, lane):
    return total_of(jnp.where(lane < W, x, 0.0))


def first_up_kernel(idx_ref, a_ref, tiles_ref, mean_ref, p_ref, sums_ref, xs, tiles, some_p, acc, held, sems):
    i = pl.program_id(0)
    lane = lane_of((1, T))

    @pl.when(i == 0)
    def _():
        for k in range(STEPS):
            tile_fetch(tiles_ref, tiles, sems, k).start()
        acc[...] = jnp.zeros_like(acc)
        spread(a_ref, lane, lambda at, x: keep_both(xs, at, H, x))

    tile_fetch(tiles_ref, tiles, sems, i).wait()

    for g in range(G):
        row = i * G + g
        rows = pl.ds(pl.multiple_of(row * T, T), T)
        p = hop_nat(row, [tiles[row, k] for k in range(KT)], idx_ref, xs).astype(bf16).astype(f32)
        some_p[g * T : (g + 1) * T, :] = p
        a = xs[rows, :].astype(f32)
        acc[0] += fold8(p * a)
        acc[1] += fold8(a * a)

    @pl.when(i == 0)
    def _():
        ratio = 2.0 * counted(acc[0], lane) / jnp.maximum(counted(acc[1], lane), 1e-30)
        held[...] = jnp.broadcast_to((ratio + mean_ref[0:1, 0:1]).astype(bf16).astype(f32), held.shape)

    center = held[0:1, :]
    for t in range(NU):
        x = packed(some_p, t, lane)
        marked = jnp.where(lane >= FREE_LANE, center, x[FREE : FREE + S])
        p_ref[t] = jnp.concatenate([x[:FREE], marked, x[FREE + S :]], axis=0).astype(bf16)

    @pl.when(i == STEPS - 1)
    def _():
        sub = lax.broadcasted_iota(jnp.int32, (8, T), 0)
        sums_ref[...] = jnp.where(sub == 0, counted(acc[0], lane), center)


def second_up_kernel(idx_ref, a_ref, p_ref, *refs):
    tiles, refs = refs[:KT], refs[KT:]
    occ_rows_ref, occ_cols_ref, sums_ref, q_ref, out_ref, xs, some_q, flat, acc = refs
    i = pl.program_id(0)
    lane = lane_of((1, T))

    @pl.when(i == 0)
    def _():
        acc[...] = jnp.zeros_like(acc)
        center = sums_ref[1:2, :]

        def open_p(s, c):
            flat[pl.ds(pl.multiple_of(s * W, 8), W), :] = unpacked(p_ref[s], lane).astype(f32)
            return c

        lax.fori_loop(0, NU * ND, open_p, 0)

        def keep(at, a):
            a = a.astype(f32)
            rows = pl.ds(at, H)
            diag = coupling * jnp.dot(occ_rows_ref[rows, :], occ_cols_ref[...], preferred_element_type=f32)
            acc[...] += fold8(diag * a * a)
            keep_both(xs, at, H, (flat[rows, :] + (diag - center) * a).astype(bf16))

        spread(a_ref, lane, keep)
        out_ref[...] = jnp.broadcast_to(sums_ref[0:1, :] + counted(acc[...], lane), out_ref.shape)

    for g in range(G):
        some_q[g * T : (g + 1) * T, :] = hop_nat(i * G + g, [tile_ref[g, 0] for tile_ref in tiles], idx_ref, xs)
    for t in range(NU):
        q_ref[t] = packed(some_q, t, lane).astype(bf16)


def pieces_in(o):
    found = []
    for u in range(NU):
        lo, hi = max(u * W, o * T), min((u + 1) * W, (o + 1) * T)
        if lo < hi:
            found.append((u, hi - o * T))
    return found


def assembled(rolled, o, lane):
    found = pieces_in(o)
    value = rolled[found[-1][0]]
    for u, end in reversed(found[:-1]):
        value = jnp.where(lane < end, rolled[u], value)
    return value


def down_kernel(idx_ref, *refs):
    pieces, refs = refs[:ND], refs[ND:]
    p_ref, tiles_ref, occ_rows_ref, occ_cols_ref = refs[:4]
    a_ref, u_ref, brief_ref, t_ref, sums_ref, tiles, xs, some_r, some_u, some_t, acc, sems = refs[4:]
    i = pl.program_id(0)
    lane = lane_of((1, T))

    @pl.when(i == 0)
    def _():
        for k in range(STEPS):
            tile_fetch(tiles_ref, tiles, sems, k).start()
        acc[...] = jnp.zeros_like(acc)
        down = idx_ref[NT * KT]
        y, z = down // NZ, lax.rem(down, NZ)
        for s in range(ND):
            source = (y if s < NZ else 1 - y) * NZ + lax.rem(z + NZ - s % NZ, NZ)
            for o in range(G):
                x = pieces[s][:, o * T : (o + 1) * T]
                xs[source * G + o] = x
                xs[NT + source * G + o] = -x

    @pl.when(i < STEPS)
    def _():
        tile_fetch(tiles_ref, tiles, sems, i).wait()
        for g in range(G):
            row = i * G + g
            r = hop_turned(row, idx_ref, tiles, xs)
            some_r[row] = r
            a = xs[row]
            a_ref[0, :, g * T : (g + 1) * T] = a
            acc[2] += fold8(r * a.astype(f32))

    @pl.when(i == STEPS)
    def _():
        def first(d, c):
            rolled, centers = {}, {}
            for o in range(G):
                for u, _end in pieces_in(o):
                    if u in rolled:
                        continue
                    x = p_ref[u * ND + d]
                    mark = x[FREE : FREE + S, :].astype(f32)[0:1, :]
                    centers[u] = jnp.sum(jnp.where(lane == FREE_LANE, mark, 0.0), axis=1, keepdims=True)
                    rolled[u] = turned(unpacked(x, lane), u * W)
                p = assembled(rolled, o, lane).astype(f32)
                center = assembled(centers, o, lane)
                at = d * G + o
                a = xs[at].astype(f32)
                diag = coupling * jnp.dot(
                    occ_rows_ref[...], occ_cols_ref[d, :, o * T : (o + 1) * T], preferred_element_type=f32
                )
                w = p + some_r[at] + diag * a
                some_u[at] = w
                some_t[at] = center * p + diag * w
                xs[NT + at] = p.astype(bf16)
                acc[0] += fold8(w * a)
                acc[1] += fold8(a * a)
            return c

        lax.fori_loop(0, ND, first, 0)
        center = total_of(acc[0]) / jnp.maximum(total_of(acc[1]), 1e-30)

        def second(d, c):
            for o in range(G):
                at = d * G + o
                w = some_u[at]
                a = xs[at].astype(f32)
                u = w - center * a
                acc[3] += fold8(u * u)
                acc[4] += fold8(u * a)
                some_u[at] = u
                some_t[at] += center * (some_r[at] - w - u)
                x = (u + xs[NT + at].astype(f32)).astype(bf16)
                xs[at] = x
                xs[NT + at] = -x
            return c

        lax.fori_loop(0, ND, second, 0)
        sub = lax.broadcasted_iota(jnp.int32, (8, T), 0)
        found = center
        for k, n in enumerate([2, 3, 4, 1]):
            found = jnp.where(sub == k + 1, total_of(acc[n]), found)
        sums_ref[...] = jnp.broadcast_to(found, sums_ref.shape)

    @pl.when(i >= STEPS)
    def _():
        for g in range(G):
            row = (i - STEPS) * G + g
            lanes = slice(g * T, (g + 1) * T)
            u = some_u[row]
            u_ref[0, :, lanes] = u
            brief_ref[0, :, lanes] = u.astype(bf16)
            t_ref[0, :, lanes] = some_t[row] + hop_turned(row, idx_ref, tiles, xs)


def joined_kernel(*refs):
    far_refs, (q_ref, up_ref, down_ref, g_ref, sums_ref, a_ref, u_ref, t_ref, sems, acc) = refs[:3], refs[3:]
    i = pl.program_id(0)
    lane = lane_of((1, T))

    def fetch(n, d):
        return pltpu.make_async_copy(far_refs[n].at[d], (a_ref, u_ref, t_ref)[n].at[d], sems.at[n, d])

    @pl.when(i == 0)
    def _():
        for d in range(ND):
            for n in range(3):
                fetch(n, d).start()

    for n in range(3):
        fetch(n, i).wait()

    @pl.when(i == 0)
    def _():
        acc[...] = jnp.zeros_like(acc)

    rolled = {}
    for o in range(G):
        for u, _end in pieces_in(o):
            if u not in rolled:
                rolled[u] = turned(unpacked(q_ref[u * ND + i], lane), u * W)
        lanes = slice(o * T, (o + 1) * T)
        a = a_ref[i, :, lanes].astype(f32)
        u = u_ref[i, :, lanes].astype(f32)
        g = assembled(rolled, o, lane).astype(f32) + t_ref[i, :, lanes]
        g_ref[i, :, lanes] = g
        for k, product in enumerate([g * g, g * u, g * a]):
            acc[k] += fold8(product)

    @pl.when(i == ND - 1)
    def _():
        row = down_ref[0:1, :]
        for k, value in enumerate(
            [down_ref[2:3, :], down_ref[3:4, :], down_ref[4:5, :]]
            + [total_of(acc[k]) for k in range(3)]
            + [up_ref[0:1, :] + down_ref[1:2, :]]
        ):
            row = jnp.where(lane == k, value, row)
        sums_ref[...] = jnp.broadcast_to(row, sums_ref.shape)


def final_kernel(a_ref, u_ref, g_ref, center_ref, shared_ref, v_ref, out_ref, coef, ready, sems):
    i = pl.program_id(0)
    lane = lane_of((1, T))

    @pl.when(i == 0)
    def _():
        table = shared_ref[...].T
        uu, ua, aa, gg, gu, ga, energy, center = [table[k : k + 1, :] for k in range(8)]

        def total(x):
            return jnp.sum(x, axis=1, keepdims=True)

        norm = total(aa)
        scale2 = 1.0 / jnp.maximum(norm, 1.0)
        alpha1 = total(energy) * scale2
        off = center - alpha1
        hh = total(gg + 4.0 * off * (gu + off * (uu + off * ua)) + off * off * (2.0 * ga + off * off * aa))
        hu = total(gu + off * (2.0 * uu + ga + off * (3.0 * ua + off * aa)))
        ha = total(ga + off * (2.0 * ua + off * aa))
        uu = total(uu + off * (2.0 * ua + off * aa))
        ua = total(ua + off * aa)
        square1 = jnp.maximum(scale2 * uu, 1.0)
        ratio2 = scale2 / square1
        alpha2 = ratio2 * (hu + alpha1 * uu - square1 * ua)
        move = alpha2 - alpha1
        nn = hh + square1 * square1 * norm + move * move * uu
        nn = nn - 2.0 * square1 * ha - 2.0 * move * hu + 2.0 * square1 * move * ua
        square2 = jnp.maximum(ratio2 * nn, 1.0)
        beta1, beta2 = jnp.sqrt(square1), jnp.sqrt(square2)
        cg = jnp.sqrt(ratio2) / beta2
        off = center_ref[0:1, 0:1] - alpha1
        row = jnp.zeros((1, T), f32)
        for k, value in enumerate(
            [alpha1, alpha2, beta1, beta2, cg * (off * (off - move) - square1), cg * (2.0 * off - move), cg]
        ):
            row = jnp.where(lane == k, value, row)
        coef[...] = jnp.broadcast_to(row, coef.shape)
        out_ref[...] = jnp.broadcast_to(row, out_ref.shape)

    ca, cu, cg = coef[0:1, 4:5], coef[0:1, 5:6], coef[0:1, 6:7]
    ready[i] = (cg * g_ref[i] + cu * u_ref[i] + ca * a_ref[i].astype(f32)).astype(bf16)

    def send(d):
        return pltpu.make_async_copy(ready.at[d], v_ref.at[d], sems.at[d])

    send(i).start()

    @pl.when(i == ND - 1)
    def _():
        for d in range(ND):
            send(d).wait()


def swapped_down(start_vector):
    y, z = lax.axis_index("dn_0"), lax.axis_index("dn_1")
    pieces = []
    for b in range(2):
        for s in range(NZ):
            to = (y if b == 0 else 1 - y) * NZ + (z + s) % NZ
            piece = lax.dynamic_slice_in_dim(start_vector, to * W, W, 0)
            if b or s:
                swaps = [(k, (k // NZ ^ b) * NZ + (k + s) % NZ) for k in range(ND)]
                piece = lax.ppermute(piece, DN, swaps)
            pieces.append(piece)
    return pieces


def body(start_vector, hop_tiles, tile_columns, tile_signs, occupation):
    rows, cols = start_vector.shape
    index = (tile_columns + NT * tile_signs).astype(jnp.int32).reshape(-1)
    up = lax.axis_index(UP)
    down = lax.axis_index(DN)
    index = jnp.concatenate([index, down.astype(jnp.int32)[None]])
    occ = occupation.astype(bf16)
    occ_rows = occ.T
    a_cols = lax.dynamic_slice_in_dim(occ, down * cols + up * W, W, 1)
    a_cols = jnp.pad(a_cols, ((0, 0), (0, T - W)))
    filled = jnp.sum(occ, axis=1, dtype=f32) * jnp.sum(a_cols, axis=1, dtype=f32)
    mean = jnp.full((8, T), coupling * jnp.sum(filled) / (occ.shape[1] * W), f32)
    b_rows = lax.dynamic_slice_in_dim(occ_rows, up * rows + down * W, W, 0)
    b_cols = jnp.moveaxis(occ.reshape(occ.shape[0], ND, cols), 1, 0)

    parts = pl.pallas_call(
        pack_kernel,
        grid=(PARTS,),
        in_specs=[pl.BlockSpec(memory_space=pl.ANY)],
        out_specs=pl.BlockSpec(memory_space=pl.ANY),
        out_shape=pltpu.HBM((NU, HEAD, T), bf16),
        scratch_shapes=[
            pltpu.VMEM(start_vector.shape, bf16),
            pltpu.VMEM((NU, HEAD, T), bf16),
            pltpu.SemaphoreType.DMA((PARTS,)),
            pltpu.SemaphoreType.DMA((NU,)),
        ],
        compiler_params=params(24),
        name="pack",
    )(far(start_vector))
    a_up = lax.all_to_all(parts, UP, 0, 0, tiled=True)
    pieces = swapped_down(start_vector)

    hop_flops = 2 * NT * KT * T * T * T
    tile_bytes = NT * KT * T * T * 2
    cost = pl.CostEstimate(flops=hop_flops, bytes_accessed=tile_bytes + 8 * 2**20, transcendentals=0)
    tall = (NT * T, T)
    packs = (NU * ND, WH, T)
    wide = (ND, W, cols)
    xs_tall = pltpu.VMEM((2 * NT * T, T), bf16)
    some = pltpu.VMEM((G * T, T), f32)

    first_up = pl.pallas_call(
        first_up_kernel,
        grid_spec=pltpu.PrefetchScalarGridSpec(
            num_scalar_prefetch=1,
            grid=(STEPS,),
            in_specs=[whole((NU, HEAD, T)), pl.BlockSpec(memory_space=pl.ANY), whole((8, T))],
            out_specs=[
                pl.BlockSpec((NU, WH, T), lambda i, *_: (i, 0, 0)),
                whole((8, T)),
            ],
            scratch_shapes=[
                xs_tall,
                pltpu.VMEM((NT, KT, T, T), bf16),
                some,
                pltpu.VMEM((2, 8, T), f32),
                pltpu.VMEM((8, T), f32),
                pltpu.SemaphoreType.DMA((STEPS,)),
            ],
        ),
        out_shape=[
            pltpu.HBM(packs, bf16),
            jax.ShapeDtypeStruct((8, T), f32),
        ],
        compiler_params=params(44),
        cost_estimate=cost,
        name="first_up",
    )
    p, sums = first_up(index, a_up, far(hop_tiles), mean)

    p_dn = lax.all_to_all(p, ALL, 0, 0, tiled=True)

    second_up = pl.pallas_call(
        second_up_kernel,
        grid_spec=pltpu.PrefetchScalarGridSpec(
            num_scalar_prefetch=1,
            grid=(STEPS,),
            in_specs=[
                whole((NU, HEAD, T)),
                whole(packs),
                *tile_specs(),
                whole(occ_rows.shape),
                whole(a_cols.shape),
                whole((8, T)),
            ],
            out_specs=[pl.BlockSpec((NU, WH, T), lambda i, *_: (i, 0, 0)), whole((8, T))],
            scratch_shapes=[xs_tall, some, pltpu.VMEM(tall, f32), pltpu.VMEM((8, T), f32)],
        ),
        out_shape=[pltpu.HBM(packs, bf16), jax.ShapeDtypeStruct((8, T), f32)],
        compiler_params=params(40),
        cost_estimate=cost,
        name="second_up",
    )
    q, up_dots = second_up(index, far(a_up), far(p), *[far(hop_tiles)] * KT, far(occ_rows), a_cols, sums)

    p_dn, q, b_cols = lax.optimization_barrier((p_dn, q, b_cols))
    q_dn = lax.all_to_all(q, ALL, 0, 0, tiled=True)

    near = pl.BlockSpec(memory_space=pltpu.VMEM)
    kept = pltpu.VMEM(wide, f32)
    cut = pltpu.VMEM((NT, W, T), f32)
    late = pl.BlockSpec((1, W, cols), lambda i, *_: (jnp.maximum(i - STEPS, 0), 0, 0))
    early = pl.BlockSpec((1, W, cols), lambda i, *_: (jnp.minimum(i, STEPS - 1), 0, 0))
    a_dn, u, brief_u, t, down_dots = pl.pallas_call(
        down_kernel,
        grid_spec=pltpu.PrefetchScalarGridSpec(
            num_scalar_prefetch=1,
            grid=(2 * STEPS,),
            in_specs=[whole((W, cols))] * ND
            + [
                whole(packs),
                pl.BlockSpec(memory_space=pl.ANY),
                whole(b_rows.shape),
                whole(b_cols.shape),
            ],
            out_specs=[early, late, late, late, whole((8, T))],
            scratch_shapes=[
                pltpu.VMEM((NT, KT, T, T), bf16),
                pltpu.VMEM((2 * NT, W, T), bf16),
                cut,
                cut,
                cut,
                pltpu.VMEM((5, 8, T), f32),
                pltpu.SemaphoreType.DMA((STEPS,)),
            ],
        ),
        out_shape=[
            pltpu.HBM(wide, bf16),
            pltpu.HBM(wide, f32),
            pltpu.HBM(wide, bf16),
            pltpu.HBM(wide, f32),
            jax.ShapeDtypeStruct((8, T), f32),
        ],
        compiler_params=params(56),
        cost_estimate=cost,
        name="down",
    )(index, *[far(x) for x in pieces], p_dn, far(hop_tiles), b_rows, b_cols)

    block = pl.BlockSpec((1, W, cols), lambda i, *_: (i, 0, 0))
    g, partial = pl.pallas_call(
        joined_kernel,
        grid=(ND,),
        in_specs=[pl.BlockSpec(memory_space=pl.ANY)] * 3 + [whole(packs), whole((8, T)), whole((8, T))],
        out_specs=[near, whole((NU * ND, T))],
        out_shape=[kept, jax.ShapeDtypeStruct((NU * ND, T), f32)],
        scratch_shapes=[
            pltpu.VMEM(wide, bf16),
            pltpu.VMEM(wide, bf16),
            pltpu.VMEM(wide, f32),
            pltpu.SemaphoreType.DMA((3, ND)),
            pltpu.VMEM((3, 8, T), f32),
        ],
        compiler_params=params(24),
        name="joined",
    )(far(a_dn), far(brief_u), far(t), q_dn, far(up_dots), far(down_dots))

    shared = lax.all_to_all(partial, ALL, 0, 0, tiled=True)
    v, scalars = pl.pallas_call(
        final_kernel,
        grid=(ND,),
        in_specs=[near, near, near, whole((8, T)), whole((NU * ND, T))],
        out_specs=[pl.BlockSpec(memory_space=pl.ANY), whole((8, T))],
        out_shape=[pltpu.HBM(wide, bf16), jax.ShapeDtypeStruct((8, T), f32)],
        scratch_shapes=[pltpu.VMEM((8, T), f32), pltpu.VMEM(wide, bf16), pltpu.SemaphoreType.DMA((ND,))],
        compiler_params=params(16),
        name="final",
    )(a_dn, u, g, far(down_dots), shared)
    final = lax.all_to_all(v, DN, 0, 0, tiled=True).reshape(rows, cols)
    return final, scalars[0, 0:2], scalars[0, 2:4]


def solution(mesh):
    torus = Mesh(mesh.devices.reshape(2, 4, 2, 2, 4), ALL)
    return jax.shard_map(
        body,
        mesh=torus,
        in_specs=(P(UP, DN), P(), P(), P(), P()),
        out_specs=(P(UP, DN), P(), P()),
        check_vma=False,
    )
```

```python
import jax
import jax.numpy as jnp
from jax import lax
from jax.experimental import pallas as pl
from jax.experimental.pallas import tpu as pltpu
from jax.sharding import Mesh
from jax.sharding import PartitionSpec as P


UP = ("up_0", "up_1", "up_2")
DN = ("dn_0", "dn_1")
ALL = UP + DN
coupling = 4.0

f32 = jnp.float32
bf16 = jnp.bfloat16

T = 128
NT = 104
KT = 5
G = 13
STEPS = NT // G
W = 104
NU = 16
ND = 8
NZ = 4
MIB = 1024 * 1024


def params(mib):
    return pltpu.CompilerParams(dimension_semantics=("arbitrary",), vmem_limit_bytes=mib * MIB)


def whole(shape):
    zeros = (0,) * len(shape)
    return pl.BlockSpec(shape, lambda i, *_: zeros, pipeline_mode=pl.Buffered(1))


def far(x):
    return pltpu.with_memory_space_constraint(x, pltpu.HBM)


def tile_specs():
    return [pl.BlockSpec((G, 1, T, T), lambda i, *_, k=k: (i, k, 0, 0)) for k in range(KT)]


def lane_of(shape):
    return lax.broadcasted_iota(jnp.int32, shape, len(shape) - 1)


def total_of(x):
    return jnp.sum(jnp.sum(x, axis=0, keepdims=True), axis=1, keepdims=True)


def fold8(x):
    return jnp.sum(x.reshape(x.shape[0] // 8, 8, x.shape[1]), axis=0)


def tile_fetch(tiles_ref, tiles, sems, k):
    rows = pl.ds(k * G, G)
    return pltpu.make_async_copy(tiles_ref.at[rows], tiles.at[rows], sems.at[k])


def hop_nat(row, lefts, idx_ref, xs):
    left = jnp.concatenate(lefts, axis=1)
    right = [xs[pl.ds(pl.multiple_of(idx_ref[row * KT + k] * T, T), T), :] for k in range(KT)]
    return jnp.dot(left, jnp.concatenate(right, axis=0), preferred_element_type=f32)


def hop_turned(row, idx_ref, tiles, xs):
    right = jnp.concatenate([tiles[row, k] for k in range(KT)], axis=1)
    left = jnp.concatenate([xs[idx_ref[row * KT + k]] for k in range(KT)], axis=1)
    return lax.dot_general(left, right, (((1,), (1,)), ((), ())), preferred_element_type=f32)


LOW = T - W
STRIPS = -(-W // LOW)


def turned(x, shift):
    shift %= T
    return pltpu.roll(x, shift, 1) if shift else x


def with_strip(head, tail, k, lane):
    return jnp.where(lane < W, head, turned(tail, W - LOW * k))


def from_strips(strips, lane):
    value = turned(strips[-1], LOW * (STRIPS - 1) - W)
    for k in reversed(range(STRIPS - 1)):
        value = jnp.where(lane < LOW * (k + 1), turned(strips[k], LOW * k - W), value)
    return value


ROWS = 832
HEAD = 704
H = 64
WH = 88
S = W - WH


PARTS = 4
ENDS = [-(-W * NU * (k + 1) // PARTS // T) * T for k in range(PARTS)]


def pack_kernel(a_ref, out_ref, near, ready, sems, out_sems):
    lane = lane_of((1, T))

    def fetch(k):
        lanes = pl.ds(ENDS[k - 1] if k else 0, ENDS[k] - (ENDS[k - 1] if k else 0))
        return pltpu.make_async_copy(a_ref.at[:, lanes], near.at[:, lanes], sems.at[k])

    def send(u):
        return pltpu.make_async_copy(ready.at[u], out_ref.at[u], out_sems.at[u])

    def cut(u, block):
        q, o = divmod(u * W, T)
        rows = slice(block * H, (block + 1) * H)
        x = turned(near[rows, q * T : (q + 1) * T], -o)
        if o + W > T:
            y = turned(near[rows, (q + 1) * T : (q + 2) * T], -o)
            x = jnp.where(lane < T - o, x, y)
        return x

    for k in range(PARTS):
        fetch(k).start()

    for k in range(PARTS):
        fetch(k).wait()
        for n in range(NU // PARTS):
            u = k * (NU // PARTS) + n
            tails = [cut(u, HEAD // H + h) for h in range(2)]
            for block in range(HEAD // H):
                x = cut(u, block)
                if block < 2 * STRIPS:
                    x = with_strip(x, tails[block % 2], block // 2, lane)
                ready[u, block * H : (block + 1) * H, :] = x
            send(u).start()
    for u in range(NU):
        send(u).wait()


def packed(values, t, lane):
    tail = values[pl.ds(pl.multiple_of(t * W, 8), S), :]
    x = values[pl.ds(pl.multiple_of(t * W + S, 8), WH), :]
    found = [with_strip(x[S * k : S * (k + 1)], tail, k, lane) for k in range(STRIPS)]
    return jnp.concatenate(found + [x[S * STRIPS :]], axis=0)


def unpacked(x, lane):
    tail = from_strips([x[S * k : S * (k + 1)] for k in range(STRIPS)], lane)
    return jnp.concatenate([tail, x], axis=0)


FREE = S * (STRIPS - 1)
FREE_LANE = W + W - LOW * (STRIPS - 1)


def spread(a_ref, lane, keep):
    def put(s, c):
        for block in range(HEAD // H):
            keep(pl.multiple_of(s * ROWS + block * H, H), a_ref[s, block * H : (block + 1) * H, :])
        for h in range(2):
            strips = [a_ref[s, (2 * k + h) * H : (2 * k + h + 1) * H, :] for k in range(STRIPS)]
            keep(pl.multiple_of(s * ROWS + HEAD + h * H, H), from_strips(strips, lane))
        return c

    lax.fori_loop(0, NU, put, 0, unroll=2)


def keep_both(xs, at, n, x):
    xs[pl.ds(at, n), :] = x
    xs[pl.ds(NT * T + at, n), :] = -x


def counted(x, lane):
    return total_of(jnp.where(lane < W, x, 0.0))


def first_up_kernel(idx_ref, a_ref, tiles_ref, mean_ref, p_ref, sums_ref, xs, tiles, some_p, acc, held, sems):
    i = pl.program_id(0)
    lane = lane_of((1, T))

    @pl.when(i == 0)
    def _():
        for k in range(STEPS):
            tile_fetch(tiles_ref, tiles, sems, k).start()
        acc[...] = jnp.zeros_like(acc)
        spread(a_ref, lane, lambda at, x: keep_both(xs, at, H, x))

    tile_fetch(tiles_ref, tiles, sems, i).wait()

    for g in range(G):
        row = i * G + g
        rows = pl.ds(pl.multiple_of(row * T, T), T)
        p = hop_nat(row, [tiles[row, k] for k in range(KT)], idx_ref, xs).astype(bf16).astype(f32)
        some_p[g * T : (g + 1) * T, :] = p
        a = xs[rows, :].astype(f32)
        acc[0] += fold8(p * a)
        acc[1] += fold8(a * a)

    @pl.when(i == 0)
    def _():
        ratio = 2.0 * counted(acc[0], lane) / jnp.maximum(counted(acc[1], lane), 1e-30)
        held[...] = jnp.broadcast_to((ratio + mean_ref[0:1, 0:1]).astype(bf16).astype(f32), held.shape)

    center = held[0:1, :]
    for t in range(NU):
        x = packed(some_p, t, lane)
        marked = jnp.where(lane >= FREE_LANE, center, x[FREE : FREE + S])
        p_ref[t] = jnp.concatenate([x[:FREE], marked, x[FREE + S :]], axis=0).astype(bf16)

    @pl.when(i == STEPS - 1)
    def _():
        sub = lax.broadcasted_iota(jnp.int32, (8, T), 0)
        sums_ref[...] = jnp.where(sub == 0, counted(acc[0], lane), center)


def second_up_kernel(idx_ref, a_ref, p_ref, *refs):
    tiles, refs = refs[:KT], refs[KT:]
    occ_rows_ref, occ_cols_ref, sums_ref, q_ref, out_ref, xs, some_q, flat, acc = refs
    i = pl.program_id(0)
    lane = lane_of((1, T))

    @pl.when(i == 0)
    def _():
        acc[...] = jnp.zeros_like(acc)
        center = sums_ref[1:2, :]

        def open_p(s, c):
            flat[pl.ds(pl.multiple_of(s * W, 8), W), :] = unpacked(p_ref[s], lane).astype(f32)
            return c

        lax.fori_loop(0, NU * ND, open_p, 0)

        def keep(at, a):
            a = a.astype(f32)
            rows = pl.ds(at, H)
            diag = coupling * jnp.dot(occ_rows_ref[rows, :], occ_cols_ref[...], preferred_element_type=f32)
            acc[...] += fold8(diag * a * a)
            keep_both(xs, at, H, (flat[rows, :] + (diag - center) * a).astype(bf16))

        spread(a_ref, lane, keep)
        out_ref[...] = jnp.broadcast_to(sums_ref[0:1, :] + counted(acc[...], lane), out_ref.shape)

    for g in range(G):
        some_q[g * T : (g + 1) * T, :] = hop_nat(i * G + g, [tile_ref[g, 0] for tile_ref in tiles], idx_ref, xs)
    for t in range(NU):
        q_ref[t] = packed(some_q, t, lane).astype(bf16)


def pieces_in(o):
    found = []
    for u in range(NU):
        lo, hi = max(u * W, o * T), min((u + 1) * W, (o + 1) * T)
        if lo < hi:
            found.append((u, hi - o * T))
    return found


def assembled(rolled, o, lane):
    found = pieces_in(o)
    value = rolled[found[-1][0]]
    for u, end in reversed(found[:-1]):
        value = jnp.where(lane < end, rolled[u], value)
    return value


def down_kernel(idx_ref, *refs):
    pieces, refs = refs[:ND], refs[ND:]
    p_ref, tiles_ref, occ_rows_ref, occ_cols_ref = refs[:4]
    a_ref, u_ref, brief_ref, t_ref, sums_ref, tiles, xs, some_r, some_u, some_t, acc, sems = refs[4:]
    i = pl.program_id(0)
    lane = lane_of((1, T))

    @pl.when(i == 0)
    def _():
        for k in range(STEPS):
            tile_fetch(tiles_ref, tiles, sems, k).start()
        acc[...] = jnp.zeros_like(acc)
        down = idx_ref[NT * KT]
        y, z = down // NZ, lax.rem(down, NZ)
        for s in range(ND):
            source = (y if s < NZ else 1 - y) * NZ + lax.rem(z + NZ - s % NZ, NZ)
            for o in range(G):
                x = pieces[s][:, o * T : (o + 1) * T]
                xs[source * G + o] = x
                xs[NT + source * G + o] = -x

    @pl.when(i < STEPS)
    def _():
        tile_fetch(tiles_ref, tiles, sems, i).wait()
        for g in range(G):
            row = i * G + g
            r = hop_turned(row, idx_ref, tiles, xs)
            some_r[row] = r
            a = xs[row]
            a_ref[0, :, g * T : (g + 1) * T] = a
            acc[2] += fold8(r * a.astype(f32))

    @pl.when(i == STEPS)
    def _():
        def first(d, c):
            rolled, centers = {}, {}
            for o in range(G):
                for u, _end in pieces_in(o):
                    if u in rolled:
                        continue
                    x = p_ref[u * ND + d]
                    mark = x[FREE : FREE + S, :].astype(f32)[0:1, :]
                    centers[u] = jnp.sum(jnp.where(lane == FREE_LANE, mark, 0.0), axis=1, keepdims=True)
                    rolled[u] = turned(unpacked(x, lane), u * W)
                p = assembled(rolled, o, lane).astype(f32)
                center = assembled(centers, o, lane)
                at = d * G + o
                a = xs[at].astype(f32)
                diag = coupling * jnp.dot(
                    occ_rows_ref[...], occ_cols_ref[d, :, o * T : (o + 1) * T], preferred_element_type=f32
                )
                w = p + some_r[at] + diag * a
                some_u[at] = w
                some_t[at] = center * p + diag * w
                xs[NT + at] = p.astype(bf16)
                acc[0] += fold8(w * a)
                acc[1] += fold8(a * a)
            return c

        lax.fori_loop(0, ND, first, 0)
        center = total_of(acc[0]) / jnp.maximum(total_of(acc[1]), 1e-30)

        def second(d, c):
            for o in range(G):
                at = d * G + o
                w = some_u[at]
                a = xs[at].astype(f32)
                u = w - center * a
                acc[3] += fold8(u * u)
                acc[4] += fold8(u * a)
                some_u[at] = u
                some_t[at] += center * (some_r[at] - w - u)
                x = (u + xs[NT + at].astype(f32)).astype(bf16)
                xs[at] = x
                xs[NT + at] = -x
            return c

        lax.fori_loop(0, ND, second, 0)
        sub = lax.broadcasted_iota(jnp.int32, (8, T), 0)
        found = center
        for k, n in enumerate([2, 3, 4, 1]):
            found = jnp.where(sub == k + 1, total_of(acc[n]), found)
        sums_ref[...] = jnp.broadcast_to(found, sums_ref.shape)

    @pl.when(i >= STEPS)
    def _():
        for g in range(G):
            row = (i - STEPS) * G + g
            lanes = slice(g * T, (g + 1) * T)
            u = some_u[row]
            u_ref[0, :, lanes] = u
            brief_ref[0, :, lanes] = u.astype(bf16)
            t_ref[0, :, lanes] = some_t[row] + hop_turned(row, idx_ref, tiles, xs)


def joined_kernel(*refs):
    far_refs, (q_ref, up_ref, down_ref, g_ref, sums_ref, a_ref, u_ref, t_ref, sems, acc) = refs[:3], refs[3:]
    lane = lane_of((1, T))

    def fetch(n, d):
        return pltpu.make_async_copy(far_refs[n].at[d], (a_ref, u_ref, t_ref)[n].at[d], sems.at[n, d])

    for d in range(ND):
        for n in range(3):
            fetch(n, d).start()

    acc[...] = jnp.zeros_like(acc)

    def join(i, c):
        for n in range(3):
            fetch(n, i).wait()
        rolled = {}
        for o in range(G):
            for u, _end in pieces_in(o):
                if u not in rolled:
                    rolled[u] = turned(unpacked(q_ref[u * ND + i], lane), u * W)
            lanes = slice(o * T, (o + 1) * T)
            a = a_ref[i, :, lanes].astype(f32)
            u = u_ref[i, :, lanes].astype(f32)
            g = assembled(rolled, o, lane).astype(f32) + t_ref[i, :, lanes]
            g_ref[i, :, lanes] = g
            for k, product in enumerate([g * g, g * u, g * a]):
                acc[k] += fold8(product)
        return c

    lax.fori_loop(0, ND, join, 0)
    row = down_ref[0:1, :]
    for k, value in enumerate(
        [down_ref[2:3, :], down_ref[3:4, :], down_ref[4:5, :]]
        + [total_of(acc[k]) for k in range(3)]
        + [up_ref[0:1, :] + down_ref[1:2, :]]
    ):
        row = jnp.where(lane == k, value, row)
    sums_ref[...] = jnp.broadcast_to(row, sums_ref.shape)


def final_kernel(a_ref, u_ref, g_ref, center_ref, shared_ref, v_ref, out_ref, coef, ready, sems):
    lane = lane_of((1, T))

    table = shared_ref[...].T
    uu, ua, aa, gg, gu, ga, energy, center = [table[k : k + 1, :] for k in range(8)]

    def total(x):
        return jnp.sum(x, axis=1, keepdims=True)

    norm = total(aa)
    scale2 = 1.0 / jnp.maximum(norm, 1.0)
    alpha1 = total(energy) * scale2
    off = center - alpha1
    hh = total(gg + 4.0 * off * (gu + off * (uu + off * ua)) + off * off * (2.0 * ga + off * off * aa))
    hu = total(gu + off * (2.0 * uu + ga + off * (3.0 * ua + off * aa)))
    ha = total(ga + off * (2.0 * ua + off * aa))
    uu = total(uu + off * (2.0 * ua + off * aa))
    ua = total(ua + off * aa)
    square1 = jnp.maximum(scale2 * uu, 1.0)
    ratio2 = scale2 / square1
    alpha2 = ratio2 * (hu + alpha1 * uu - square1 * ua)
    move = alpha2 - alpha1
    nn = hh + square1 * square1 * norm + move * move * uu
    nn = nn - 2.0 * square1 * ha - 2.0 * move * hu + 2.0 * square1 * move * ua
    square2 = jnp.maximum(ratio2 * nn, 1.0)
    beta1, beta2 = jnp.sqrt(square1), jnp.sqrt(square2)
    cg = jnp.sqrt(ratio2) / beta2
    off = center_ref[0:1, 0:1] - alpha1
    row = jnp.zeros((1, T), f32)
    for k, value in enumerate(
        [alpha1, alpha2, beta1, beta2, cg * (off * (off - move) - square1), cg * (2.0 * off - move), cg]
    ):
        row = jnp.where(lane == k, value, row)
    coef[...] = jnp.broadcast_to(row, coef.shape)
    out_ref[...] = jnp.broadcast_to(row, out_ref.shape)

    ca, cu, cg = coef[0:1, 4:5], coef[0:1, 5:6], coef[0:1, 6:7]

    def send(d):
        return pltpu.make_async_copy(ready.at[d], v_ref.at[d], sems.at[d])

    def combine(d, c):
        ready[d] = (cg * g_ref[d] + cu * u_ref[d] + ca * a_ref[d].astype(f32)).astype(bf16)
        send(d).start()
        return c

    lax.fori_loop(0, ND, combine, 0)
    for d in range(ND):
        send(d).wait()


def swapped_down(start_vector):
    y, z = lax.axis_index("dn_0"), lax.axis_index("dn_1")
    pieces = []
    for b in range(2):
        for s in range(NZ):
            to = (y if b == 0 else 1 - y) * NZ + (z + s) % NZ
            piece = lax.dynamic_slice_in_dim(start_vector, to * W, W, 0)
            if b or s:
                swaps = [(k, (k // NZ ^ b) * NZ + (k + s) % NZ) for k in range(ND)]
                piece = lax.ppermute(piece, DN, swaps)
            pieces.append(piece)
    return pieces


def body(start_vector, hop_tiles, tile_columns, tile_signs, occupation):
    rows, cols = start_vector.shape
    index = (tile_columns + NT * tile_signs).astype(jnp.int32).reshape(-1)
    up = lax.axis_index(UP)
    down = lax.axis_index(DN)
    index = jnp.concatenate([index, down.astype(jnp.int32)[None]])
    occ = occupation.astype(bf16)
    occ_rows = occ.T
    a_cols = lax.dynamic_slice_in_dim(occ, down * cols + up * W, W, 1)
    a_cols = jnp.pad(a_cols, ((0, 0), (0, T - W)))
    filled = jnp.sum(occ, axis=1, dtype=f32) * jnp.sum(a_cols, axis=1, dtype=f32)
    mean = jnp.full((8, T), coupling * jnp.sum(filled) / (occ.shape[1] * W), f32)
    b_rows = lax.dynamic_slice_in_dim(occ_rows, up * rows + down * W, W, 0)
    b_cols = jnp.moveaxis(occ.reshape(occ.shape[0], ND, cols), 1, 0)

    parts = pl.pallas_call(
        pack_kernel,
        in_specs=[pl.BlockSpec(memory_space=pl.ANY)],
        out_specs=pl.BlockSpec(memory_space=pl.ANY),
        out_shape=pltpu.HBM((NU, HEAD, T), bf16),
        scratch_shapes=[
            pltpu.VMEM(start_vector.shape, bf16),
            pltpu.VMEM((NU, HEAD, T), bf16),
            pltpu.SemaphoreType.DMA((PARTS,)),
            pltpu.SemaphoreType.DMA((NU,)),
        ],
        compiler_params=pltpu.CompilerParams(vmem_limit_bytes=24 * MIB),
        name="pack",
    )(far(start_vector))
    a_up = lax.all_to_all(parts, UP, 0, 0, tiled=True)
    pieces = swapped_down(start_vector)

    hop_flops = 2 * NT * KT * T * T * T
    tile_bytes = NT * KT * T * T * 2
    cost = pl.CostEstimate(flops=hop_flops, bytes_accessed=tile_bytes + 8 * 2**20, transcendentals=0)
    tall = (NT * T, T)
    packs = (NU * ND, WH, T)
    wide = (ND, W, cols)
    xs_tall = pltpu.VMEM((2 * NT * T, T), bf16)
    some = pltpu.VMEM((G * T, T), f32)

    first_up = pl.pallas_call(
        first_up_kernel,
        grid_spec=pltpu.PrefetchScalarGridSpec(
            num_scalar_prefetch=1,
            grid=(STEPS,),
            in_specs=[whole((NU, HEAD, T)), pl.BlockSpec(memory_space=pl.ANY), whole((8, T))],
            out_specs=[
                pl.BlockSpec((NU, WH, T), lambda i, *_: (i, 0, 0)),
                whole((8, T)),
            ],
            scratch_shapes=[
                xs_tall,
                pltpu.VMEM((NT, KT, T, T), bf16),
                some,
                pltpu.VMEM((2, 8, T), f32),
                pltpu.VMEM((8, T), f32),
                pltpu.SemaphoreType.DMA((STEPS,)),
            ],
        ),
        out_shape=[
            pltpu.HBM(packs, bf16),
            jax.ShapeDtypeStruct((8, T), f32),
        ],
        compiler_params=params(44),
        cost_estimate=cost,
        name="first_up",
    )
    p, sums = first_up(index, a_up, far(hop_tiles), mean)

    p_dn = lax.all_to_all(p, ALL, 0, 0, tiled=True)

    second_up = pl.pallas_call(
        second_up_kernel,
        grid_spec=pltpu.PrefetchScalarGridSpec(
            num_scalar_prefetch=1,
            grid=(STEPS,),
            in_specs=[
                whole((NU, HEAD, T)),
                whole(packs),
                *tile_specs(),
                whole(occ_rows.shape),
                whole(a_cols.shape),
                whole((8, T)),
            ],
            out_specs=[pl.BlockSpec((NU, WH, T), lambda i, *_: (i, 0, 0)), whole((8, T))],
            scratch_shapes=[xs_tall, some, pltpu.VMEM(tall, f32), pltpu.VMEM((8, T), f32)],
        ),
        out_shape=[pltpu.HBM(packs, bf16), jax.ShapeDtypeStruct((8, T), f32)],
        compiler_params=params(40),
        cost_estimate=cost,
        name="second_up",
    )
    q, up_dots = second_up(index, far(a_up), far(p), *[far(hop_tiles)] * KT, far(occ_rows), a_cols, sums)

    p_dn, q, b_cols = lax.optimization_barrier((p_dn, q, b_cols))
    q_dn = lax.all_to_all(q, ALL, 0, 0, tiled=True)

    near = pl.BlockSpec(memory_space=pltpu.VMEM)
    kept = pltpu.VMEM(wide, f32)
    cut = pltpu.VMEM((NT, W, T), f32)
    late = pl.BlockSpec((1, W, cols), lambda i, *_: (jnp.maximum(i - STEPS, 0), 0, 0))
    early = pl.BlockSpec((1, W, cols), lambda i, *_: (jnp.minimum(i, STEPS - 1), 0, 0))
    a_dn, u, brief_u, t, down_dots = pl.pallas_call(
        down_kernel,
        grid_spec=pltpu.PrefetchScalarGridSpec(
            num_scalar_prefetch=1,
            grid=(2 * STEPS,),
            in_specs=[whole((W, cols))] * ND
            + [
                whole(packs),
                pl.BlockSpec(memory_space=pl.ANY),
                whole(b_rows.shape),
                whole(b_cols.shape),
            ],
            out_specs=[early, late, late, late, whole((8, T))],
            scratch_shapes=[
                pltpu.VMEM((NT, KT, T, T), bf16),
                pltpu.VMEM((2 * NT, W, T), bf16),
                cut,
                cut,
                cut,
                pltpu.VMEM((5, 8, T), f32),
                pltpu.SemaphoreType.DMA((STEPS,)),
            ],
        ),
        out_shape=[
            pltpu.HBM(wide, bf16),
            pltpu.HBM(wide, f32),
            pltpu.HBM(wide, bf16),
            pltpu.HBM(wide, f32),
            jax.ShapeDtypeStruct((8, T), f32),
        ],
        compiler_params=params(56),
        cost_estimate=cost,
        name="down",
    )(index, *[far(x) for x in pieces], p_dn, far(hop_tiles), b_rows, b_cols)

    block = pl.BlockSpec((1, W, cols), lambda i, *_: (i, 0, 0))
    g, partial = pl.pallas_call(
        joined_kernel,
        grid=(1,),
        in_specs=[pl.BlockSpec(memory_space=pl.ANY)] * 3 + [whole(packs), whole((8, T)), whole((8, T))],
        out_specs=[near, whole((NU * ND, T))],
        out_shape=[kept, jax.ShapeDtypeStruct((NU * ND, T), f32)],
        scratch_shapes=[
            pltpu.VMEM(wide, bf16),
            pltpu.VMEM(wide, bf16),
            pltpu.VMEM(wide, f32),
            pltpu.SemaphoreType.DMA((3, ND)),
            pltpu.VMEM((3, 8, T), f32),
        ],
        compiler_params=params(24),
        name="joined",
    )(far(a_dn), far(brief_u), far(t), q_dn, far(up_dots), far(down_dots))

    shared = lax.all_to_all(partial, ALL, 0, 0, tiled=True)
    v, scalars = pl.pallas_call(
        final_kernel,
        grid=(1,),
        in_specs=[near, near, near, whole((8, T)), whole((NU * ND, T))],
        out_specs=[pl.BlockSpec(memory_space=pl.ANY), whole((8, T))],
        out_shape=[pltpu.HBM(wide, bf16), jax.ShapeDtypeStruct((8, T), f32)],
        scratch_shapes=[pltpu.VMEM((8, T), f32), pltpu.VMEM(wide, bf16), pltpu.SemaphoreType.DMA((ND,))],
        compiler_params=params(16),
        name="final",
    )(a_dn, u, g, far(down_dots), shared)
    final = lax.all_to_all(v, DN, 0, 0, tiled=True).reshape(rows, cols)
    return final, scalars[0, 0:2], scalars[0, 2:4]


def solution(mesh):
    torus = Mesh(mesh.devices.reshape(2, 4, 2, 2, 4), ALL)
    return jax.shard_map(
        body,
        mesh=torus,
        in_specs=(P(UP, DN), P(), P(), P(), P()),
        out_specs=(P(UP, DN), P(), P()),
        check_vma=False,
    )
```
